256 devices in a mesh: shard: 32 (over y, x, core), dp: 8 (over z).
Axes of the slice: x: 4, y: 4, z: 8, core: 2. Of those that a mesh axis runs over, the one named last changes fastest.
Arguments:
- grad: float32 [288, 128, 4096], P('shard', 'dp'), may hold values from -252 to 252
- param: bfloat16 [288, 128, 4096], P('shard', 'dp'), may hold values from -0.119628906 to 0.119628906
- row_state: float32 [288, 128], P('shard', 'dp'), may hold values from 0.3 to 27
- col_state: float32 [3, 4096], replicated, may hold values from 0.002 to 400
- block_start: int32 [32], replicated, may hold values from 0 to 143, as said below
- block_matrix: int32 [144], replicated, may hold values from 0 to 2, as said below
- step: int32 [1], replicated, may hold values from 2 to 11
Outputs:
- new_params: bfloat16 [18432, 4096], P(None, 'shard')
- new_row_state: float32 [288, 128], P('shard', 'dp')
- new_col_state: float32 [3, 4096], replicated
The draws below stay inside these ranges and needn't reach their ends.
Inputs may be any that keep to these rules, and one draw needn't show every extreme that they name: block_start rises from 0 at index 0; every shard index owns between 1 and 9 consecutive global blocks, held in its first slots, and some index owns exactly 9; slots past a device's owned count hold values that no output reads. `block_matrix`: ids 0 and 1 each label 4096 / 128 blocks and id 2 labels 10240 / 128 blocks, in any order.
All inputs are finite; a program needn't handle non-finite values.
Results may differ from the reference program's by a relative error of at most 0.0004.
Values may be sent and summed in bfloat16 or wider, within the bound.
No kernel may reach another device: no remote copies, remote signals or barrier semaphores. Data moves between devices by JAX's collectives and lax.ppermute only.
A program may use at most 64 MiB of HBM per device.

```python
import math
import jax
import jax.numpy as jnp
from jax import lax

D = 4096
FF = 10240
BLOCK = 128
MATS = 3
NB = 144
CAP = 9
N_SHARD = 32


def draw_grad(key, part):
    noise_key, row_key, col_key = jax.random.split(jax.random.fold_in(key, 11), 3)
    slot_total = N_SHARD * CAP
    draw_base = jnp.clip(jax.random.normal(noise_key, (slot_total, BLOCK, D), jnp.float32), -4.0, 4.0)
    row_scale = jnp.exp(jax.random.uniform(row_key, (slot_total, BLOCK), jnp.float32, math.log(0.3), math.log(3.0)))
    col_scale = jnp.exp(jax.random.uniform(col_key, (D,), jnp.float32, math.log(0.3), math.log(3.0)))
    position = jnp.arange(slot_total, dtype=jnp.float32) / max(slot_total - 1, 1)
    ramp_scale = 1.0 + 2.0 * position
    return draw_base * (row_scale * ramp_scale[:, None])[:, :, None] * col_scale[None, None, :]


def draw_row_state(key, part):
    slot_total = N_SHARD * CAP
    state_key = jax.random.fold_in(key, 23)
    position = jnp.arange(slot_total, dtype=jnp.float32) / max(slot_total - 1, 1)
    values = jnp.exp(jax.random.uniform(state_key, (slot_total, BLOCK), jnp.float32, math.log(0.3), math.log(3.0)))
    ramp_scale = 1.0 + 2.0 * position
    return values * ramp_scale[:, None]


def draw_col_state(key, part):
    state_key = jax.random.fold_in(key, 37)
    lowest = jnp.array([0.002, 64.0, 0.002], jnp.float32)
    factor = jnp.exp(jax.random.uniform(state_key, (MATS, D), jnp.float32, 0.0, math.log(4.0)))
    return lowest[:, None] * factor


def draw_block_matrix(key, part):
    order_key = jax.random.fold_in(key, 41)
    block_index = jnp.arange(NB, dtype=jnp.int32)
    first_end = D // BLOCK
    second_end = 2 * (D // BLOCK)
    labels = (block_index >= first_end).astype(jnp.int32) + (block_index >= second_end).astype(jnp.int32)
    return jax.random.permutation(order_key, labels).astype(jnp.int32)


def draw_block_start(key, part):
    busy_key, move_key = jax.random.split(jax.random.fold_in(key, 53))
    busy_device = jax.random.randint(busy_key, (), 0, N_SHARD - 1)
    last_device = N_SHARD - 1
    rest_blocks = NB - CAP - 1
    base_count = rest_blocks // (N_SHARD - 2)
    extra_count = rest_blocks % (N_SHARD - 2)
    device_ids = jnp.arange(N_SHARD, dtype=jnp.int32)
    position_rank = device_ids - (device_ids > busy_device).astype(jnp.int32)
    spread_count = base_count + (position_rank < extra_count).astype(jnp.int32)
    counts = jnp.where(device_ids == busy_device, CAP, jnp.where(device_ids == last_device, 1, spread_count)).astype(jnp.int32)

    def move(turn, counts):
        turn_key = jax.random.fold_in(move_key, turn)
        pair_key, amount_key = jax.random.split(turn_key)
        ends_pair = jax.random.randint(pair_key, (2,), 0, N_SHARD)
        source = ends_pair[0]
        target = ends_pair[1]
        wanted = jax.random.randint(amount_key, (), 0, CAP)
        usable = (source != busy_device) & (target != busy_device) & (source != target) & (source != last_device) & (target != last_device)
        amount = jnp.minimum(jnp.minimum(wanted, counts[source] - 1), CAP - counts[target])
        amount = jnp.where(usable, jnp.maximum(amount, 0), 0).astype(jnp.int32)
        return counts.at[source].add(-amount).at[target].add(amount)
    counts = lax.fori_loop(0, 4 * N_SHARD, move, counts)
    return (jnp.cumsum(counts) - counts).astype(jnp.int32)


def levels(stream_key, dims, pieces, least, largest):
    gain = 1.0
    for axis_at, parts in pieces:
        draws = jax.random.uniform(jax.random.fold_in(jax.random.fold_in(stream_key, 6), axis_at), (parts,), jnp.float32, least / len(pieces), largest / len(pieces))
        gain = gain * jnp.repeat(jnp.exp(draws), dims[axis_at] // parts).reshape((-1,) + (1,) * (len(dims) - 1 - axis_at))
    return gain


def normal_values(stream_key, shape, width, limit, shards=(), kind=jnp.bfloat16):
    values = width * jax.random.normal(stream_key, shape, jnp.float32)
    if shards:
        values = values * levels(stream_key, shape, shards, -0.22, 0.18)
    return jnp.clip(values, -limit, limit).astype(kind)


def setup_inputs(seed: int = 0) -> dict:
    streams_of = jax.random.split(jax.random.key(seed), 8)
    return {
        "grad": draw_grad(jax.random.fold_in(streams_of[7], 71), 0),
        "param": normal_values(streams_of[1], (N_SHARD * CAP, BLOCK, D), 0.02, 0.119628906, ((0, 32), (1, 8))),
        "row_state": draw_row_state(jax.random.fold_in(streams_of[7], 71), 0),
        "col_state": draw_col_state(jax.random.fold_in(streams_of[7], 71), 0),
        "block_start": draw_block_start(jax.random.fold_in(streams_of[7], 71), 0),
        "block_matrix": draw_block_matrix(jax.random.fold_in(streams_of[7], 71), 0),
        "step": jax.random.randint(streams_of[6], (1,), 2, 12).astype(jnp.int32),
    }


def scale_grad(grad, safe_rows, matrix_pick, new_cols, row_avg):
    slot_cols = jnp.dot(matrix_pick, new_cols, precision=lax.Precision.HIGHEST)
    slot_avg = jnp.dot(matrix_pick, row_avg, precision=lax.Precision.HIGHEST)
    return grad / jnp.sqrt(safe_rows[:, :, None] * slot_cols[:, None, :] / slot_avg[:, None, None])

def reference(grad, param, row_state, col_state, block_start, block_matrix, step):
    slot_total = grad.shape[0]
    block_ends = jnp.concatenate([block_start[1:], jnp.full((1,), NB, jnp.int32)])
    slot_ids = jnp.arange(slot_total, dtype=jnp.int32)
    owner_shard = slot_ids // CAP
    within = slot_ids % CAP
    owned_count = (block_ends - block_start)[owner_shard]
    live_slot = within < owned_count
    block_ids = jnp.minimum(block_start[owner_shard] + within, NB - 1).astype(jnp.int32)
    matrix_ids = jnp.where(live_slot, block_matrix[block_ids], 0)
    matrix_pick = (matrix_ids[:, None] == jnp.arange(3, dtype=jnp.int32)[None, :]).astype(jnp.float32)
    member = matrix_pick * live_slot[:, None].astype(jnp.float32)
    row_count = jnp.array([D, D, FF], jnp.float32)
    step_value = step[0].astype(jnp.float32)
    decay_rate = 1.0 - step_value ** (-0.8)
    learn_rate = 1.0 / jnp.sqrt(jnp.maximum(step_value, 10000.0))
    squares = grad * grad
    new_rows = jnp.where(live_slot[:, None], decay_rate * row_state + (1.0 - decay_rate) * lax.optimization_barrier(jnp.sum(squares, axis=2)) / D, 0.0)
    safe_rows = jnp.where(live_slot[:, None], new_rows, 1.0)
    col_total = jnp.einsum('sm,sd->md', member, lax.optimization_barrier(jnp.sum(squares, axis=1)), precision=lax.Precision.HIGHEST)
    new_cols = decay_rate * col_state + (1.0 - decay_rate) * col_total / row_count[:, None]
    row_avg = jnp.dot(lax.optimization_barrier(jnp.sum(new_rows, axis=1)), member, precision=lax.Precision.HIGHEST) / row_count
    scaled = scale_grad(grad, safe_rows, matrix_pick, new_cols, row_avg)
    square_total = jnp.dot(lax.optimization_barrier(jnp.sum(scaled * scaled, axis=(1, 2))), member, precision=lax.Precision.HIGHEST)
    clip_factor = jnp.maximum(1.0, jnp.sqrt(square_total / (row_count * D)))
    slot_clip = jnp.dot(matrix_pick, clip_factor, precision=lax.Precision.HIGHEST)
    updated = jnp.where(live_slot[:, None, None], param.astype(jnp.float32) - learn_rate * scaled / slot_clip[:, None, None], 0.0).astype(jnp.bfloat16)
    block_index = jnp.arange(NB, dtype=jnp.int32)
    block_owner = lax.optimization_barrier(jnp.sum((block_start[None, :] <= block_index[:, None]).astype(jnp.int32), axis=1)) - 1
    slot_of = (block_owner * CAP + block_index - jnp.take(block_start, block_owner)).astype(jnp.int32)
    new_params = jnp.take(updated, slot_of, axis=0).reshape(NB * BLOCK, D)
    return (new_params, new_rows, new_cols)
```

```python
import functools

import jax
import jax.numpy as jnp
from jax import lax
from jax.experimental import pallas as pl
from jax.experimental.pallas import tpu as pltpu
from jax.sharding import Mesh
from jax.sharding import PartitionSpec as P

D = 4096
FF = 10240
ROWS = (D, D, FF)
MATS = 3
NB = 144
CAP = 9
N_SHARD = 32
SUB = 16
LANES = 128
TILES = D // LANES
HALF = D // 2
HALF_NB = NB // 2
DP = 8
SHARD = ("shard_0", "shard_1", "shard_2")
F32 = jnp.float32
BF16 = jnp.bfloat16


SMEM = pl.BlockSpec(memory_space=pltpu.SMEM)
VMEM = pl.BlockSpec(memory_space=pltpu.VMEM)
ANY = pl.BlockSpec(memory_space=pl.ANY)


def owned_range(start_ref):
    shard = (lax.axis_index("shard_0") * 4 + lax.axis_index("shard_1")) * 2 + lax.axis_index("shard_2")
    first = start_ref[shard]
    end = jnp.where(shard == N_SHARD - 1, NB, start_ref[jnp.minimum(shard + 1, N_SHARD - 1)])
    return first, end - first


def decay_rate(step_ref, shape):
    t = jnp.full(shape, step_ref[0].astype(F32))
    return 1.0 - jnp.exp(-0.8 * jnp.log(t))


def diagonal():
    shape = (SUB, SUB)
    return lax.broadcasted_iota(jnp.int32, shape, 0) == lax.broadcasted_iota(jnp.int32, shape, 1)


def to_column(row, eye):
    return jnp.sum(jnp.where(eye, jnp.broadcast_to(row, (SUB, SUB)), 0.0), axis=1, keepdims=True)


def to_row(column, eye):
    return jnp.sum(jnp.where(eye, jnp.broadcast_to(column, (SUB, SUB)), 0.0), axis=0, keepdims=True)


def tile(c):
    return slice(c * LANES, (c + 1) * LANES)


def stats_kernel(
    start_ref, matrix_ref, step_ref, grad_ref, row_state_ref,
    mine_ref, theirs_ref, new_rows_ref,
    held, sums, row_sums, inverse, row_total, sems,
):
    first, owned = owned_range(start_ref)

    def fetch(s):
        return pltpu.make_async_copy(grad_ref.at[s], held.at[s], sems.at[s])

    @pl.loop(0, owned)
    def _(s):
        fetch(s).start()

    sums[...] = jnp.zeros_like(sums)
    row_total[...] = jnp.zeros_like(row_total)

    @pl.loop(0, owned)
    def _(s):
        fetch(s).wait()
        total = jnp.zeros((SUB, LANES), F32)
        for c in range(TILES):
            x = held[s, :, tile(c)]
            total = total + x * x
        row_sums[s] = total

    eye = diagonal()
    decay = decay_rate(step_ref, (SUB, 1))
    for s in range(CAP):
        mean = jnp.sum(row_sums[s], axis=1, keepdims=True) / D
        state = to_column(row_state_ref[s : s + 1, :], eye)
        new = jnp.where(s < owned, decay * state + (1.0 - decay) * mean, 0.0)
        new_rows_ref[s : s + 1, :] = to_row(new, eye)
        inverse[s] = jnp.broadcast_to(jnp.where(s < owned, 1.0 / new, 0.0), (SUB, LANES))
        row_sums[s] = jnp.broadcast_to(new, (SUB, LANES))

    @pl.loop(0, owned)
    def _(s):
        m = matrix_ref[first + s]
        inv = inverse[s]
        new = row_sums[s]
        row_total[m] += new[:8] + new[8:]
        for c in range(TILES):
            x = held[s, :, tile(c)]
            sq = x * x
            quot = sq * inv
            sums[m, :, tile(c)] += sq[:8] + sq[8:]
            sums[MATS + m, :, tile(c)] += quot[:8] + quot[8:]

    core = lax.axis_index("shard_2")
    for ref, half in ((mine_ref, core), (theirs_ref, 1 - core)):
        ref[...] = jnp.zeros_like(ref)
        cols = pl.ds(pl.multiple_of(half * HALF, HALF), HALF)
        for m in range(MATS):
            ref[m : m + 1, :] = jnp.sum(sums[m, :, cols], axis=0, keepdims=True)
            ref[4 + m : 5 + m, :] = jnp.sum(sums[MATS + m, :, cols], axis=0, keepdims=True)
            ref[3:4, tile(m)] = jnp.sum(row_total[m], axis=0, keepdims=True)


def stats(block_start, block_matrix, step, grad, row_state):
    part = jax.ShapeDtypeStruct((8, HALF), F32)
    return pl.pallas_call(
        stats_kernel,
        out_shape=(part, part, jax.ShapeDtypeStruct((CAP, SUB), F32)),
        in_specs=[SMEM, SMEM, SMEM, ANY, VMEM],
        out_specs=(VMEM, VMEM, VMEM),
        scratch_shapes=[
            pltpu.VMEM((CAP, SUB, D), F32),
            pltpu.VMEM((2 * MATS, 8, D), F32),
            pltpu.VMEM((CAP, SUB, LANES), F32),
            pltpu.VMEM((CAP, SUB, LANES), F32),
            pltpu.VMEM((MATS, 8, LANES), F32),
            pltpu.SemaphoreType.DMA((CAP,)),
        ],
        name="stats",
    )(block_start, block_matrix, step, grad, row_state)


def update_kernel(
    start_ref, matrix_ref, step_ref, grad_ref, param_ref, new_rows_ref, mine_ref, theirs_ref, col_state_ref,
    out_ref, new_cols_ref,
    held, held_param, factor, inverse, sems,
):
    first, owned = owned_range(start_ref)

    def fetch(s):
        return (
            pltpu.make_async_copy(grad_ref.at[s], held.at[s], sems.at[0, s]),
            pltpu.make_async_copy(param_ref.at[s], held_param.at[s], sems.at[1, s]),
        )

    @pl.loop(0, owned)
    def _(s):
        for copy in fetch(s):
            copy.start()

    south = lax.axis_index("shard_2") == 0
    decay = decay_rate(step_ref, (1, 1))
    t = jnp.full((1, 1), step_ref[0].astype(F32))
    learn_rate = 1.0 / jnp.sqrt(jnp.maximum(t, 10000.0))
    for m in range(MATS):
        weight = jnp.zeros((1, 1), F32)
        roots = []
        row_avg = jnp.where(south, mine_ref[3:4, tile(m)], theirs_ref[3:4, tile(m)])[:, :1] / ROWS[m]
        for half in range(2):
            a, b = (mine_ref, theirs_ref) if half == 0 else (theirs_ref, mine_ref)
            col = jnp.where(south, a[m : m + 1, :], b[m : m + 1, :])
            quot = jnp.where(south, a[4 + m : 5 + m, :], b[4 + m : 5 + m, :])
            cols = slice(half * HALF, (half + 1) * HALF)
            new = decay * col_state_ref[m : m + 1, cols] + (1.0 - decay) * col / ROWS[m]
            new_cols_ref[m : m + 1, cols] = new
            weight = weight + jnp.sum(quot / new, axis=1, keepdims=True)
            roots.append(1.0 / jnp.sqrt(new))
        clip = jnp.maximum(1.0, jnp.sqrt(row_avg * weight / (ROWS[m] * float(D))))
        scale = learn_rate * jnp.sqrt(row_avg) / clip
        for half in range(2):
            cols = slice(half * HALF, (half + 1) * HALF)
            factor[m, :, cols] = jnp.broadcast_to(roots[half] * scale, (8, HALF))

    eye = diagonal()
    for s in range(CAP):
        new = to_column(new_rows_ref[s : s + 1, :], eye)
        inverse[s] = jnp.broadcast_to(1.0 / jnp.sqrt(jnp.where(s < owned, new, 1.0)), (SUB, LANES))

    @pl.loop(0, owned)
    def _(s):
        for copy in fetch(s):
            copy.wait()
        m = matrix_ref[first + s]
        inv = inverse[s]
        for c in range(TILES):
            f = factor[m, :, tile(c)]
            change = held[s, :, tile(c)] * inv * jnp.concatenate([f, f], axis=0)
            out_ref[c, s] = (held_param[s, :, tile(c)].astype(F32) - change).astype(BF16)


def update(block_start, block_matrix, step, grad, param, new_rows, mine, theirs, col_state):
    return pl.pallas_call(
        update_kernel,
        out_shape=(
            jax.ShapeDtypeStruct((N_SHARD, CAP, SUB, LANES), BF16),
            jax.ShapeDtypeStruct((MATS, D), F32),
        ),
        in_specs=[SMEM, SMEM, SMEM, ANY, ANY, VMEM, VMEM, VMEM, VMEM],
        out_specs=(VMEM, VMEM),
        scratch_shapes=[
            pltpu.VMEM((CAP, SUB, D), F32),
            pltpu.VMEM((CAP, SUB, D), BF16),
            pltpu.VMEM((MATS, 8, D), F32),
            pltpu.VMEM((CAP, SUB, LANES), F32),
            pltpu.SemaphoreType.DMA((2, CAP)),
        ],
        name="update",
    )(block_start, block_matrix, step, grad, param, new_rows, mine, theirs, col_state)


def pack_kernel(start_ref, slots_ref, low_ref, high_ref):
    owner = jnp.int32(0)
    for ref, base in ((low_ref, 0), (high_ref, HALF_NB)):

        def place(k, owner, ref=ref, base=base):
            b = base + k
            later = start_ref[jnp.minimum(owner + 1, N_SHARD - 1)]
            owner = jnp.where((owner < N_SHARD - 1) & (b >= later), owner + 1, owner)
            ref[k] = slots_ref[owner, b - start_ref[owner]]
            return owner

        owner = lax.fori_loop(0, HALF_NB, place, owner)


def pack(block_start, slots):
    part = jax.ShapeDtypeStruct((HALF_NB, SUB, LANES), BF16)
    return pl.pallas_call(
        pack_kernel,
        out_shape=(part, part),
        in_specs=[SMEM, VMEM],
        out_specs=(VMEM, VMEM),
        name="pack",
    )(block_start, slots)


def place_kernel(where, *refs):
    pieces, out_ref, sems = refs[: len(where)], refs[-2], refs[-1]
    at = lax.axis_index("dp")
    copies = []
    for k, ((half, behind), piece) in enumerate(zip(where, pieces)):
        source = lax.rem(at + (DP - behind) % DP, DP)
        target = out_ref.at[
            pl.ds(half * HALF_NB, HALF_NB), pl.ds(pl.multiple_of(source * SUB, SUB), SUB), :
        ]
        copies.append(pltpu.make_async_copy(piece, target, sems.at[k]))
    for copy in copies:
        copy.start()
    for copy in copies:
        copy.wait()


def place(where, pieces, out=None):
    n = len(pieces)
    return pl.pallas_call(
        functools.partial(place_kernel, where),
        out_shape=jax.ShapeDtypeStruct((NB, DP * SUB, LANES), BF16),
        in_specs=[VMEM] * n + ([] if out is None else [ANY]),
        out_specs=ANY,
        scratch_shapes=[pltpu.SemaphoreType.DMA((n,))],
        input_output_aliases={} if out is None else {n: 0},
        name="place",
    )(*pieces, *(() if out is None else (out,)))


def moved(x, axis, by):
    n = lax.axis_size(axis)
    return lax.ppermute(x, axis, [(i, (i + by) % n) for i in range(n)])


def summed_over_4(x, axis):
    a, b, c = (moved(x, axis, k) for k in (1, 3, 2))
    return (x + c) + (a + b)


def summed_over_8(x, axis):
    p = {k: moved(x, axis, k) for k in (1, 7, 2, 6, 3, 5, 4)}
    return ((x + p[4]) + (p[2] + p[6])) + ((p[1] + p[5]) + (p[3] + p[7]))


def body(grad, param, row_state, col_state, block_start, block_matrix, step):
    mine, theirs, new_rows = stats(block_start, block_matrix, step, grad, row_state)
    mine = mine + moved(theirs, "shard_2", 1)
    mine = summed_over_4(mine, "shard_1")
    mine = summed_over_4(mine, "shard_0")
    mine = summed_over_8(mine, "dp")
    theirs = moved(mine, "shard_2", 1)
    slots, new_cols = update(
        block_start, block_matrix, step, grad, param, new_rows, mine, theirs, col_state
    )
    slots = lax.all_to_all(slots, SHARD, 0, 0, tiled=True)
    halves = pack(block_start, slots)
    held = {(0, 0): halves[0], (1, 0): halves[1]}
    for hop in range(1, DP // 2 + 1):
        for half, way in ((0, 1), (0, -1), (1, 1), (1, -1)):
            if hop == DP // 2 and way != (1 if half == 0 else -1):
                continue
            held[half, way * hop] = moved(held[half, way * (hop - 1)], "dp", way)
    early = [k for k in held if abs(k[1]) <= 2]
    late = [k for k in held if abs(k[1]) > 2]
    out = place(tuple(early), [held[k] for k in early])
    out = place(tuple(late), [held[k] for k in late], out)
    return (out.reshape(NB * DP * SUB, LANES), new_rows, new_cols)


def solution(mesh):
    finer = Mesh(
        mesh.devices.reshape(4, 4, 2, mesh.shape["dp"]), ("shard_0", "shard_1", "shard_2", "dp")
    )
    in_specs = (P(SHARD, "dp", None), P(SHARD, "dp", None), P(SHARD, "dp"), P(), P(), P(), P())
    out_specs = (P(None, SHARD), P(SHARD, "dp"), P())
    return jax.shard_map(body, mesh=finer, in_specs=in_specs, out_specs=out_specs, check_vma=False)
```

```python
import functools

import jax
import jax.numpy as jnp
from jax import lax
from jax.experimental import pallas as pl
from jax.experimental.pallas import tpu as pltpu
from jax.sharding import Mesh
from jax.sharding import PartitionSpec as P


D = 4096
FF = 10240
ROWS = (D, D, FF)
MATS = 3
NB = 144
CAP = 9
N_SHARD = 32
SUB = 16
LANES = 128
TILES = D // LANES
PIECE = SUB // 2
DP = 8
SHARD = ("shard_0", "shard_1", "shard_2")
F32 = jnp.float32
BF16 = jnp.bfloat16


SMEM = pl.BlockSpec(memory_space=pltpu.SMEM)
VMEM = pl.BlockSpec(memory_space=pltpu.VMEM)
ANY = pl.BlockSpec(memory_space=pl.ANY)
MOST_VMEM = 62 << 20


def owned_range(start_ref):
    shard = (lax.axis_index("shard_0") * 4 + lax.axis_index("shard_1")) * 2 + lax.axis_index("shard_2")
    first = start_ref[shard]
    end = jnp.where(shard == N_SHARD - 1, NB, start_ref[jnp.minimum(shard + 1, N_SHARD - 1)])
    return first, end - first


def decay_rate(step_ref, shape):
    t = jnp.full(shape, step_ref[0].astype(F32))
    return 1.0 - jnp.exp(-0.8 * jnp.log(t))


def diagonal():
    shape = (SUB, SUB)
    return lax.broadcasted_iota(jnp.int32, shape, 0) == lax.broadcasted_iota(jnp.int32, shape, 1)


def to_column(row, eye):
    return jnp.sum(jnp.where(eye, jnp.broadcast_to(row, (SUB, SUB)), 0.0), axis=1, keepdims=True)


def to_row(column, eye):
    return jnp.sum(jnp.where(eye, jnp.broadcast_to(column, (SUB, SUB)), 0.0), axis=0, keepdims=True)


def tile(c):
    return slice(c * LANES, (c + 1) * LANES)


def stats_kernel(
    start_ref, matrix_ref, step_ref, grad_ref, row_state_ref,
    part_ref, new_rows_ref, table_ref,
    held, sums, row_sums, inverse, row_total, sems,
):
    first, owned = owned_range(start_ref)

    def fetch(s):
        return pltpu.make_async_copy(grad_ref.at[s], held.at[s], sems.at[s])

    @pl.loop(0, owned)
    def _(s):
        fetch(s).start()

    sums[...] = jnp.zeros_like(sums)
    row_total[...] = jnp.zeros_like(row_total)
    shape = (8, LANES)
    block = lax.broadcasted_iota(jnp.int32, shape, 0) * LANES + lax.broadcasted_iota(jnp.int32, shape, 1)
    slot = block
    for d in range(1, N_SHARD):
        slot = slot + jnp.where(block >= start_ref[d], CAP - (start_ref[d] - start_ref[d - 1]), 0)
    table_ref[...] = slot

    @pl.loop(0, owned)
    def _(s):
        fetch(s).wait()
        total = jnp.zeros((SUB, LANES), F32)
        for c in range(TILES):
            x = held[s, :, tile(c)]
            total = total + x * x
        row_sums[s] = total

    eye = diagonal()
    decay = decay_rate(step_ref, (SUB, 1))
    for s in range(CAP):
        mean = jnp.sum(row_sums[s], axis=1, keepdims=True) / D
        state = to_column(row_state_ref[s : s + 1, :], eye)
        new = jnp.where(s < owned, decay * state + (1.0 - decay) * mean, 0.0)
        new_rows_ref[s : s + 1, :] = to_row(new, eye)
        inverse[s] = jnp.broadcast_to(jnp.where(s < owned, 1.0 / new, 0.0), (SUB, LANES))
        row_sums[s] = jnp.broadcast_to(new, (SUB, LANES))

    @pl.loop(0, owned)
    def _(s):
        m = matrix_ref[first + s]
        inv = inverse[s]
        new = row_sums[s]
        row_total[m] += new[:8] + new[8:]
        for c in range(TILES):
            x = held[s, :, tile(c)]
            sq = x * x
            quot = sq * inv
            sums[m, :, tile(c)] += sq[:8] + sq[8:]
            sums[MATS + m, :, tile(c)] += quot[:8] + quot[8:]

    for c in range(TILES):
        for m in range(MATS):
            part_ref[c, m : m + 1, :] = jnp.sum(sums[m, :, tile(c)], axis=0, keepdims=True)
            part_ref[c, 4 + m : 5 + m, :] = jnp.sum(sums[MATS + m, :, tile(c)], axis=0, keepdims=True)
        row = jnp.sum(row_total[c], axis=0, keepdims=True) if c < MATS else jnp.zeros((1, LANES), F32)
        part_ref[c, 3:4, :] = row
        part_ref[c, 7:8, :] = jnp.zeros((1, LANES), F32)


def stats(block_start, block_matrix, step, grad, row_state):
    return pl.pallas_call(
        stats_kernel,
        out_shape=(
            jax.ShapeDtypeStruct((TILES, 8, LANES), F32),
            jax.ShapeDtypeStruct((CAP, SUB), F32),
            jax.ShapeDtypeStruct((8, LANES), jnp.int32),
        ),
        in_specs=[SMEM, SMEM, SMEM, ANY, VMEM],
        out_specs=(VMEM, VMEM, VMEM),
        scratch_shapes=[
            pltpu.VMEM((CAP, SUB, D), F32),
            pltpu.VMEM((2 * MATS, 8, D), F32),
            pltpu.VMEM((CAP, SUB, LANES), F32),
            pltpu.VMEM((CAP, SUB, LANES), F32),
            pltpu.VMEM((MATS, 8, LANES), F32),
            pltpu.SemaphoreType.DMA((CAP,)),
        ],
        compiler_params=pltpu.CompilerParams(vmem_limit_bytes=MOST_VMEM),
        cost_estimate=pl.CostEstimate(flops=4000000, bytes_accessed=2400000, transcendentals=0),
        name="stats",
    )(block_start, block_matrix, step, grad, row_state)


def update_kernel(
    half, start_ref, matrix_ref, step_ref, grad_ref, param_ref, new_rows_ref, total_ref, col_state_ref,
    out_ref, new_cols_ref,
    held, held_param, factor, inverse, sems,
):
    first, owned = owned_range(start_ref)
    rows = slice(half * PIECE, (half + 1) * PIECE)

    def fetch(s):
        return (
            pltpu.make_async_copy(grad_ref.at[s, rows, :], held.at[s], sems.at[0, s]),
            pltpu.make_async_copy(param_ref.at[s, rows, :], held_param.at[s], sems.at[1, s]),
        )

    @pl.loop(0, owned)
    def _(s):
        for copy in fetch(s):
            copy.start()

    matrix = lax.broadcasted_iota(jnp.int32, (MATS, 1), 0)
    count = jnp.where(matrix == 2, float(ROWS[2]), float(ROWS[0]))
    decay = decay_rate(step_ref, (MATS, 1))
    t = jnp.full((MATS, 1), step_ref[0].astype(F32))
    learn_rate = 1.0 / jnp.sqrt(jnp.maximum(t, 10000.0))
    row_avg = jnp.where(
        matrix == 0, total_ref[0, 3:4, :1], jnp.where(matrix == 1, total_ref[1, 3:4, :1], total_ref[2, 3:4, :1])
    ) / count
    weight = jnp.zeros((MATS, LANES), F32)
    for c in range(TILES):
        new = decay * col_state_ref[:, tile(c)] + (1.0 - decay) * total_ref[c, :MATS, :] / count
        new_cols_ref[:, tile(c)] = new
        weight = weight + total_ref[c, 4 : 4 + MATS, :] / new
    weight = jnp.sum(weight, axis=1, keepdims=True)
    clip = jnp.maximum(1.0, jnp.sqrt(row_avg * weight / (count * float(D))))
    scale = learn_rate * jnp.sqrt(row_avg) / clip
    for c in range(TILES):
        root = scale / jnp.sqrt(new_cols_ref[:, tile(c)])
        for m in range(MATS):
            factor[m, :, tile(c)] = jnp.broadcast_to(root[m : m + 1, :], (8, LANES))

    eye = diagonal()
    for s in range(CAP):
        new = to_column(new_rows_ref[s : s + 1, :], eye)[rows]
        inverse[s] = jnp.broadcast_to(1.0 / jnp.sqrt(jnp.where(s < owned, new, 1.0)), (PIECE, LANES))

    @pl.loop(0, owned)
    def _(s):
        for copy in fetch(s):
            copy.wait()
        m = matrix_ref[first + s]
        inv = inverse[s]
        for c in range(TILES):
            change = held[s, :, tile(c)] * inv * factor[m, :, tile(c)]
            out_ref[c, s] = (held_param[s, :, tile(c)].astype(F32) - change).astype(BF16)


def update(half, block_start, block_matrix, step, grad, param, new_rows, total, col_state):
    return pl.pallas_call(
        functools.partial(update_kernel, half),
        out_shape=(
            jax.ShapeDtypeStruct((N_SHARD, CAP, PIECE, LANES), BF16),
            jax.ShapeDtypeStruct((MATS, D), F32),
        ),
        in_specs=[SMEM, SMEM, SMEM, ANY, ANY, VMEM, VMEM, VMEM],
        out_specs=(VMEM, VMEM),
        scratch_shapes=[
            pltpu.VMEM((CAP, PIECE, D), F32),
            pltpu.VMEM((CAP, PIECE, D), BF16),
            pltpu.VMEM((MATS, 8, D), F32),
            pltpu.VMEM((CAP, PIECE, LANES), F32),
            pltpu.SemaphoreType.DMA((2, CAP)),
        ],
        compiler_params=pltpu.CompilerParams(vmem_limit_bytes=MOST_VMEM),
        cost_estimate=pl.CostEstimate(flops=4000000, bytes_accessed=2400000, transcendentals=0),
        name="update",
    )(block_start, block_matrix, step, grad, param, new_rows, total, col_state)


def pack_kernel(table_ref, slots_ref, out_ref):
    for b in range(NB):
        out_ref[b] = slots_ref[table_ref[b // LANES, b % LANES]]


def pack(table, slots):
    return pl.pallas_call(
        pack_kernel,
        out_shape=jax.ShapeDtypeStruct((NB, PIECE, LANES), BF16),
        in_specs=[SMEM, VMEM],
        out_specs=VMEM,
        compiler_params=pltpu.CompilerParams(vmem_limit_bytes=4 << 20),
        cost_estimate=pl.CostEstimate(flops=2000000, bytes_accessed=1200000, transcendentals=0),
        name="pack",
    )(table, slots.reshape(N_SHARD * CAP, PIECE, LANES))


def place_kernel(where, *refs):
    pieces, out_ref, sems = refs[: len(where)], refs[-2], refs[-1]
    at = lax.axis_index("dp")
    copies = []
    for k, ((half, behind), piece) in enumerate(zip(where, pieces)):
        source = lax.rem(at + (DP - behind) % DP, DP)
        row = pl.multiple_of(source * SUB + half * PIECE, PIECE)
        copies.append(pltpu.make_async_copy(piece, out_ref.at[:, pl.ds(row, PIECE), :], sems.at[k]))
    for copy in copies:
        copy.start()
    for copy in copies:
        copy.wait()


def place(where, pieces, out=None):
    n = len(pieces)
    return pl.pallas_call(
        functools.partial(place_kernel, where),
        out_shape=jax.ShapeDtypeStruct((NB, DP * SUB, LANES), BF16),
        in_specs=[ANY] * (n if out is None else n + 1),
        out_specs=ANY,
        scratch_shapes=[pltpu.SemaphoreType.DMA((n,))],
        input_output_aliases={} if out is None else {n: 0},
        compiler_params=pltpu.CompilerParams(vmem_limit_bytes=1 << 20),
        cost_estimate=pl.CostEstimate(flops=2000000, bytes_accessed=2400000, transcendentals=0),
        name="place",
    )(*pieces, *(() if out is None else (out,)))


def moved(x, axis, by):
    n = lax.axis_size(axis)
    return lax.ppermute(x, axis, [(i, (i + by) % n) for i in range(n)])


def sent_to_all(x, axes, n):
    return lax.all_to_all(jnp.broadcast_to(x, (n, *x.shape)), axes, 0, 0, tiled=True)


def summed(part):
    tiles = ("shard_1", "dp")
    own = jnp.sum(lax.all_to_all(part, tiles, 0, 0, tiled=True), axis=0)
    own = jnp.sum(sent_to_all(own, ("shard_0", "shard_2"), 8), axis=0)
    return sent_to_all(own, tiles, TILES)


def steps(grad, param, row_state, col_state, block_start, block_matrix, step):
    part, new_rows, table = stats(block_start, block_matrix, step, grad, row_state)
    total = summed(part)
    slots = []
    for half in range(2):
        moving, cols = update(
            half, block_start, block_matrix, step, grad, param, new_rows, total, col_state
        )
        if half == 0:
            new_cols = cols
        slots.append(lax.all_to_all(moving, SHARD, 0, 0, tiled=True))
    held = {}
    for half in range(2):
        held[half, 0] = pack(table, slots[half])
    for hop in range(1, DP // 2 + 1):
        for half, way in ((0, 1), (0, -1), (1, 1), (1, -1)):
            if hop == DP // 2 and way != (1 if half == 0 else -1):
                continue
            held[half, way * hop] = moved(held[half, way * (hop - 1)], "dp", way)
    early = [k for k in held if abs(k[1]) <= 2]
    late = [k for k in held if abs(k[1]) > 2]
    out = place(tuple(early), [held[k] for k in early])
    out = place(tuple(late), [held[k] for k in late], out)
    return (out.reshape(NB * DP * SUB, LANES), new_rows, new_cols)


def solution(mesh):
    finer = Mesh(
        mesh.devices.reshape(4, 4, 2, mesh.shape["dp"]), ("shard_0", "shard_1", "shard_2", "dp")
    )
    in_specs = (P(SHARD, "dp", None), P(SHARD, "dp", None), P(SHARD, "dp"), P(), P(), P(), P())
    out_specs = (P(None, SHARD), P(SHARD, "dp"), P())
    return jax.shard_map(steps, mesh=finer, in_specs=in_specs, out_specs=out_specs, check_vma=False)
```

```python
import functools

import jax
import jax.numpy as jnp
from jax import lax
from jax.experimental import pallas as pl
from jax.experimental.pallas import tpu as pltpu
from jax.sharding import Mesh
from jax.sharding import PartitionSpec as P

D = 4096
FF = 10240
ROWS = (D, D, FF)
MATS = 3
NB = 144
CAP = 9
N_SHARD = 32
SUB = 16
LANES = 128
TILES = D // LANES
PARTS = 2
PART = NB // PARTS
DP = 8
SHARD = ("shard_0", "shard_1", "shard_2")
F32 = jnp.float32
BF16 = jnp.bfloat16


SMEM = pl.BlockSpec(memory_space=pltpu.SMEM)
VMEM = pl.BlockSpec(memory_space=pltpu.VMEM)
ANY = pl.BlockSpec(memory_space=pl.ANY)
MOST_VMEM = 62 << 20


def owned_range(start_ref):
    shard = (lax.axis_index("shard_0") * 4 + lax.axis_index("shard_1")) * 2 + lax.axis_index("shard_2")
    first = start_ref[shard]
    end = jnp.where(shard == N_SHARD - 1, NB, start_ref[jnp.minimum(shard + 1, N_SHARD - 1)])
    return first, end - first


def decay_rate(step_ref, shape):
    t = jnp.full(shape, step_ref[0].astype(F32))
    return 1.0 - jnp.exp(-0.8 * jnp.log(t))


def diagonal():
    shape = (SUB, SUB)
    return lax.broadcasted_iota(jnp.int32, shape, 0) == lax.broadcasted_iota(jnp.int32, shape, 1)


def to_column(row, eye):
    return jnp.sum(jnp.where(eye, jnp.broadcast_to(row, (SUB, SUB)), 0.0), axis=1, keepdims=True)


def to_row(column, eye):
    return jnp.sum(jnp.where(eye, jnp.broadcast_to(column, (SUB, SUB)), 0.0), axis=0, keepdims=True)


def tile(c):
    return slice(c * LANES, (c + 1) * LANES)


def stats_kernel(
    start_ref, matrix_ref, step_ref, grad_ref, row_state_ref,
    part_ref, new_rows_ref, table_ref,
    held, sums, row_sums, inverse, row_total, sems,
):
    first, owned = owned_range(start_ref)

    def fetch(s):
        return pltpu.make_async_copy(grad_ref.at[s], held.at[s], sems.at[s])

    @pl.loop(0, owned)
    def _(s):
        fetch(s).start()

    sums[...] = jnp.zeros_like(sums)
    row_total[...] = jnp.zeros_like(row_total)
    shape = (8, LANES)
    block = lax.broadcasted_iota(jnp.int32, shape, 0) * LANES + lax.broadcasted_iota(jnp.int32, shape, 1)
    slot = block
    for d in range(1, N_SHARD):
        slot = slot + jnp.where(block >= start_ref[d], CAP - (start_ref[d] - start_ref[d - 1]), 0)
    table_ref[...] = slot

    @pl.loop(0, owned)
    def _(s):
        fetch(s).wait()
        total = jnp.zeros((SUB, LANES), F32)
        for c in range(TILES):
            x = held[s, :, tile(c)]
            total = total + x * x
        row_sums[s] = total

    eye = diagonal()
    decay = decay_rate(step_ref, (SUB, 1))
    for s in range(CAP):
        mean = jnp.sum(row_sums[s], axis=1, keepdims=True) / D
        state = to_column(row_state_ref[s : s + 1, :], eye)
        new = jnp.where(s < owned, decay * state + (1.0 - decay) * mean, 0.0)
        new_rows_ref[s : s + 1, :] = to_row(new, eye)
        inverse[s] = jnp.broadcast_to(jnp.where(s < owned, 1.0 / new, 0.0), (SUB, LANES))
        row_sums[s] = jnp.broadcast_to(new, (SUB, LANES))

    @pl.loop(0, owned)
    def _(s):
        m = matrix_ref[first + s]
        inv = inverse[s]
        new = row_sums[s]
        row_total[m] += new[:8] + new[8:]
        for c in range(TILES):
            x = held[s, :, tile(c)]
            sq = x * x
            quot = sq * inv
            sums[m, :, tile(c)] += sq[:8] + sq[8:]
            sums[MATS + m, :, tile(c)] += quot[:8] + quot[8:]

    for c in range(TILES):
        for m in range(MATS):
            part_ref[c, m : m + 1, :] = jnp.sum(sums[m, :, tile(c)], axis=0, keepdims=True)
            part_ref[c, 4 + m : 5 + m, :] = jnp.sum(sums[MATS + m, :, tile(c)], axis=0, keepdims=True)
        row = jnp.sum(row_total[c], axis=0, keepdims=True) if c < MATS else jnp.zeros((1, LANES), F32)
        part_ref[c, 3:4, :] = row
        part_ref[c, 7:8, :] = jnp.zeros((1, LANES), F32)


def stats(block_start, block_matrix, step, grad, row_state):
    return pl.pallas_call(
        stats_kernel,
        out_shape=(
            jax.ShapeDtypeStruct((TILES, 8, LANES), F32),
            jax.ShapeDtypeStruct((CAP, SUB), F32),
            jax.ShapeDtypeStruct((8, LANES), jnp.int32),
        ),
        in_specs=[SMEM, SMEM, SMEM, ANY, VMEM],
        out_specs=(VMEM, VMEM, VMEM),
        scratch_shapes=[
            pltpu.VMEM((CAP, SUB, D), F32),
            pltpu.VMEM((2 * MATS, 8, D), F32),
            pltpu.VMEM((CAP, SUB, LANES), F32),
            pltpu.VMEM((CAP, SUB, LANES), F32),
            pltpu.VMEM((MATS, 8, LANES), F32),
            pltpu.SemaphoreType.DMA((CAP,)),
        ],
        compiler_params=pltpu.CompilerParams(vmem_limit_bytes=MOST_VMEM),
        cost_estimate=pl.CostEstimate(flops=4000000, bytes_accessed=2400000, transcendentals=0),
        name="stats",
    )(block_start, block_matrix, step, grad, row_state)


def update_kernel(
    start_ref, matrix_ref, step_ref, grad_ref, param_ref, new_rows_ref, total_ref, col_state_ref,
    out_ref, new_cols_ref,
    factor, inverse,
):
    first, owned = owned_range(start_ref)
    matrix = lax.broadcasted_iota(jnp.int32, (MATS, 1), 0)
    count = jnp.where(matrix == 2, float(ROWS[2]), float(ROWS[0]))
    decay = decay_rate(step_ref, (MATS, 1))
    t = jnp.full((MATS, 1), step_ref[0].astype(F32))
    learn_rate = 1.0 / jnp.sqrt(jnp.maximum(t, 10000.0))
    row_avg = jnp.where(
        matrix == 0, total_ref[0, 3:4, :1], jnp.where(matrix == 1, total_ref[1, 3:4, :1], total_ref[2, 3:4, :1])
    ) / count
    weight = jnp.zeros((MATS, LANES), F32)
    for c in range(TILES):
        new = decay * col_state_ref[:, tile(c)] + (1.0 - decay) * total_ref[c, :MATS, :] / count
        new_cols_ref[:, tile(c)] = new
        weight = weight + total_ref[c, 4 : 4 + MATS, :] / new
    weight = jnp.sum(weight, axis=1, keepdims=True)
    clip = jnp.maximum(1.0, jnp.sqrt(row_avg * weight / (count * float(D))))
    scale = learn_rate * jnp.sqrt(row_avg) / clip
    for c in range(TILES):
        root = scale / jnp.sqrt(new_cols_ref[:, tile(c)])
        for m in range(MATS):
            factor[m, :, tile(c)] = jnp.broadcast_to(root[m : m + 1, :], (8, LANES))

    eye = diagonal()
    for s in range(CAP):
        new = to_column(new_rows_ref[s : s + 1, :], eye)
        inverse[s] = jnp.broadcast_to(1.0 / jnp.sqrt(jnp.where(s < owned, new, 1.0)), (SUB, LANES))

    @pl.loop(0, owned)
    def _(s):
        m = matrix_ref[first + s]
        inv = inverse[s]
        for c in range(TILES):
            f = factor[m, :, tile(c)]
            change = grad_ref[s, :, tile(c)] * inv * jnp.concatenate([f, f], axis=0)
            out_ref[c, s] = (param_ref[s, :, tile(c)].astype(F32) - change).astype(BF16)


def update(block_start, block_matrix, step, grad, param, new_rows, total, col_state):
    return pl.pallas_call(
        update_kernel,
        out_shape=(
            jax.ShapeDtypeStruct((N_SHARD, CAP, SUB, LANES), BF16),
            jax.ShapeDtypeStruct((MATS, D), F32),
        ),
        in_specs=[SMEM, SMEM, SMEM, VMEM, VMEM, VMEM, VMEM, VMEM],
        out_specs=(VMEM, VMEM),
        scratch_shapes=[
            pltpu.VMEM((MATS, 8, D), F32),
            pltpu.VMEM((CAP, SUB, LANES), F32),
        ],
        compiler_params=pltpu.CompilerParams(vmem_limit_bytes=16 << 20),
        cost_estimate=pl.CostEstimate(flops=4000000, bytes_accessed=2400000, transcendentals=0),
        name="update",
    )(block_start, block_matrix, step, grad, param, new_rows, total, col_state)


def pack_kernel(table_ref, slots_ref, *out_refs):
    for b in range(NB):
        out_refs[b // PART][b % PART] = slots_ref[table_ref[b // LANES, b % LANES]]


def pack(table, slots):
    return pl.pallas_call(
        pack_kernel,
        out_shape=[jax.ShapeDtypeStruct((PART, SUB, LANES), BF16)] * PARTS,
        in_specs=[SMEM, VMEM],
        out_specs=[VMEM] * PARTS,
        compiler_params=pltpu.CompilerParams(vmem_limit_bytes=4 << 20),
        cost_estimate=pl.CostEstimate(flops=2000000, bytes_accessed=1200000, transcendentals=0),
        name="pack",
    )(table, slots.reshape(N_SHARD * CAP, SUB, LANES))


def place_kernel(where, *refs):
    pieces, out_ref, sems = refs[: len(where)], refs[-2], refs[-1]
    at = lax.axis_index("dp")
    copies = []
    for k, ((part, behind), piece) in enumerate(zip(where, pieces)):
        source = lax.rem(at + (DP - behind) % DP, DP)
        row = pl.multiple_of(source * SUB, SUB)
        target = out_ref.at[pl.ds(part * PART, PART), pl.ds(row, SUB), :]
        copies.append(pltpu.make_async_copy(piece, target, sems.at[k]))
    for copy in copies:
        copy.start()
    for copy in copies:
        copy.wait()


def place(where, pieces, out=None):
    n = len(pieces)
    return pl.pallas_call(
        functools.partial(place_kernel, where),
        out_shape=jax.ShapeDtypeStruct((NB, DP * SUB, LANES), BF16),
        in_specs=[ANY] * (n if out is None else n + 1),
        out_specs=ANY,
        scratch_shapes=[pltpu.SemaphoreType.DMA((n,))],
        input_output_aliases={} if out is None else {n: 0},
        compiler_params=pltpu.CompilerParams(vmem_limit_bytes=1 << 20),
        cost_estimate=pl.CostEstimate(flops=2000000, bytes_accessed=2400000, transcendentals=0),
        name="place",
    )(*pieces, *(() if out is None else (out,)))


def moved(x, axis, by):
    n = lax.axis_size(axis)
    return lax.ppermute(x, axis, [(i, (i + by) % n) for i in range(n)])


def fold_kernel(parts_ref, out_ref):
    total = parts_ref[0]
    for k in range(1, parts_ref.shape[0]):
        total = total + parts_ref[k]
    for k in range(out_ref.shape[0]):
        out_ref[k] = total


def fold(parts, copies):
    return pl.pallas_call(
        fold_kernel,
        out_shape=jax.ShapeDtypeStruct((copies, 8, LANES), F32),
        in_specs=[VMEM],
        out_specs=VMEM,
        compiler_params=pltpu.CompilerParams(vmem_limit_bytes=2 << 20),
        cost_estimate=pl.CostEstimate(flops=1000000000, bytes_accessed=4000000, transcendentals=0),
        name="fold",
    )(parts)


def summed(part):
    tiles, rest = ("shard_1", "dp"), ("shard_0", "shard_2")
    own = lax.all_to_all(part, tiles, 0, 0, tiled=True)
    own = lax.all_to_all(fold(own, N_SHARD * DP // TILES), rest, 0, 0, tiled=True)
    return lax.all_to_all(fold(own, TILES), tiles, 0, 0, tiled=True)


def body(grad, param, row_state, col_state, block_start, block_matrix, step):
    part, new_rows, table = stats(block_start, block_matrix, step, grad, row_state)
    total = summed(part)
    slots, new_cols = update(
        block_start, block_matrix, step, grad, param, new_rows, total, col_state
    )
    slots = lax.all_to_all(slots, SHARD, 0, 0, tiled=True)
    held = {}
    for part, piece in enumerate(pack(table, slots)):
        held[part, 0] = piece
    for hop in range(1, DP // 2 + 1):
        for part in range(PARTS):
            for way in (1, -1):
                if hop == DP // 2 and way != (1 if part == 0 else -1):
                    continue
                held[part, way * hop] = moved(held[part, way * (hop - 1)], "dp", way)
    early = [k for k in held if abs(k[1]) <= 2]
    late = [k for k in held if abs(k[1]) > 2]
    out = place(tuple(early), [held[k] for k in early])
    out = place(tuple(late), [held[k] for k in late], out)
    return (out.reshape(NB * DP * SUB, LANES), new_rows, new_cols)


def solution(mesh):
    finer = Mesh(
        mesh.devices.reshape(4, 4, 2, mesh.shape["dp"]), ("shard_0", "shard_1", "shard_2", "dp")
    )
    in_specs = (P(SHARD, "dp", None), P(SHARD, "dp", None), P(SHARD, "dp"), P(), P(), P(), P())
    out_specs = (P(None, SHARD), P(SHARD, "dp"), P())
    return jax.shard_map(body, mesh=finer, in_specs=in_specs, out_specs=out_specs, check_vma=False)
```

```python
import functools

import jax
import jax.numpy as jnp
from jax import lax
from jax.experimental import pallas as pl
from jax.experimental.pallas import tpu as pltpu
from jax.sharding import Mesh
from jax.sharding import PartitionSpec as P

D = 4096
FF = 10240
ROWS = (D, D, FF)
MATS = 3
NB = 144
CAP = 9
N_SHARD = 32
SUB = 16
LANES = 128
TILES = D // LANES
PARTS = 2
PART = NB // PARTS
DP = 8
SHARD = ("shard_0", "shard_1", "shard_2")
F32 = jnp.float32
BF16 = jnp.bfloat16


SMEM = pl.BlockSpec(memory_space=pltpu.SMEM)
VMEM = pl.BlockSpec(memory_space=pltpu.VMEM)
ANY = pl.BlockSpec(memory_space=pl.ANY)
MOST_VMEM = 62 << 20


def owned_range(start_ref):
    shard = (lax.axis_index("shard_0") * 4 + lax.axis_index("shard_1")) * 2 + lax.axis_index("shard_2")
    first = start_ref[shard]
    end = jnp.where(shard == N_SHARD - 1, NB, start_ref[jnp.minimum(shard + 1, N_SHARD - 1)])
    return first, end - first


def decay_rate(step_ref, shape):
    t = jnp.full(shape, step_ref[0].astype(F32))
    return 1.0 - jnp.exp(-0.8 * jnp.log(t))


def diagonal():
    shape = (SUB, SUB)
    return lax.broadcasted_iota(jnp.int32, shape, 0) == lax.broadcasted_iota(jnp.int32, shape, 1)


def to_column(row, eye):
    return jnp.sum(jnp.where(eye, jnp.broadcast_to(row, (SUB, SUB)), 0.0), axis=1, keepdims=True)


def to_row(column, eye):
    return jnp.sum(jnp.where(eye, jnp.broadcast_to(column, (SUB, SUB)), 0.0), axis=0, keepdims=True)


def tile(c):
    return slice(c * LANES, (c + 1) * LANES)


def stats_kernel(
    start_ref, matrix_ref, step_ref, grad_ref, row_state_ref,
    part_ref, new_rows_ref, table_ref,
    held, sums, row_sums, inverse, row_total, sems,
):
    first, owned = owned_range(start_ref)

    def fetch(s):
        return pltpu.make_async_copy(grad_ref.at[s], held.at[s], sems.at[s])

    @pl.loop(0, owned)
    def _(s):
        fetch(s).start()

    sums[...] = jnp.zeros_like(sums)
    row_total[...] = jnp.zeros_like(row_total)
    shape = (8, LANES)
    block = lax.broadcasted_iota(jnp.int32, shape, 0) * LANES + lax.broadcasted_iota(jnp.int32, shape, 1)
    slot = block
    for d in range(1, N_SHARD):
        slot = slot + jnp.where(block >= start_ref[d], CAP - (start_ref[d] - start_ref[d - 1]), 0)
    table_ref[...] = slot

    @pl.loop(0, owned)
    def _(s):
        fetch(s).wait()
        total = jnp.zeros((SUB, LANES), F32)
        for c in range(TILES):
            x = held[s, :, tile(c)]
            total = total + x * x
        row_sums[s] = total

    eye = diagonal()
    decay = decay_rate(step_ref, (SUB, 1))
    for s in range(CAP):
        mean = jnp.sum(row_sums[s], axis=1, keepdims=True) / D
        state = to_column(row_state_ref[s : s + 1, :], eye)
        new = jnp.where(s < owned, decay * state + (1.0 - decay) * mean, 0.0)
        new_rows_ref[s : s + 1, :] = to_row(new, eye)
        inverse[s] = jnp.broadcast_to(jnp.where(s < owned, 1.0 / new, 0.0), (SUB, LANES))
        row_sums[s] = jnp.broadcast_to(new, (SUB, LANES))

    @pl.loop(0, owned)
    def _(s):
        m = matrix_ref[first + s]
        inv = inverse[s]
        new = row_sums[s]
        row_total[m] += new[:8] + new[8:]
        for c in range(TILES):
            x = held[s, :, tile(c)]
            sq = x * x
            quot = sq * inv
            sums[m, :, tile(c)] += sq[:8] + sq[8:]
            sums[MATS + m, :, tile(c)] += quot[:8] + quot[8:]

    for c in range(TILES):
        for m in range(MATS):
            part_ref[c, m : m + 1, :] = jnp.sum(sums[m, :, tile(c)], axis=0, keepdims=True)
            part_ref[c, 4 + m : 5 + m, :] = jnp.sum(sums[MATS + m, :, tile(c)], axis=0, keepdims=True)
        row = jnp.sum(row_total[c], axis=0, keepdims=True) if c < MATS else jnp.zeros((1, LANES), F32)
        part_ref[c, 3:4, :] = row
        part_ref[c, 7:8, :] = jnp.zeros((1, LANES), F32)


def stats(block_start, block_matrix, step, grad, row_state):
    return pl.pallas_call(
        stats_kernel,
        out_shape=(
            jax.ShapeDtypeStruct((TILES, 8, LANES), F32),
            jax.ShapeDtypeStruct((CAP, SUB), F32),
            jax.ShapeDtypeStruct((8, LANES), jnp.int32),
        ),
        in_specs=[SMEM, SMEM, SMEM, ANY, VMEM],
        out_specs=(VMEM, VMEM, VMEM),
        scratch_shapes=[
            pltpu.VMEM((CAP, SUB, D), F32),
            pltpu.VMEM((2 * MATS, 8, D), F32),
            pltpu.VMEM((CAP, SUB, LANES), F32),
            pltpu.VMEM((CAP, SUB, LANES), F32),
            pltpu.VMEM((MATS, 8, LANES), F32),
            pltpu.SemaphoreType.DMA((CAP,)),
        ],
        compiler_params=pltpu.CompilerParams(vmem_limit_bytes=MOST_VMEM),
        cost_estimate=pl.CostEstimate(flops=4000000, bytes_accessed=2400000, transcendentals=0),
        name="stats",
    )(block_start, block_matrix, step, grad, row_state)


def update_kernel(
    start_ref, matrix_ref, step_ref, grad_ref, param_ref, new_rows_ref, total_ref, col_state_ref,
    out_ref, new_cols_ref,
    factor, inverse,
):
    first, owned = owned_range(start_ref)
    matrix = lax.broadcasted_iota(jnp.int32, (MATS, 1), 0)
    count = jnp.where(matrix == 2, float(ROWS[2]), float(ROWS[0]))
    decay = decay_rate(step_ref, (MATS, 1))
    t = jnp.full((MATS, 1), step_ref[0].astype(F32))
    learn_rate = 1.0 / jnp.sqrt(jnp.maximum(t, 10000.0))
    row_avg = jnp.where(
        matrix == 0, total_ref[0, 3:4, :1], jnp.where(matrix == 1, total_ref[1, 3:4, :1], total_ref[2, 3:4, :1])
    ) / count
    weight = jnp.zeros((MATS, LANES), F32)
    for c in range(TILES):
        new = decay * col_state_ref[:, tile(c)] + (1.0 - decay) * total_ref[c, :MATS, :] / count
        new_cols_ref[:, tile(c)] = new
        weight = weight + total_ref[c, 4 : 4 + MATS, :] / new
    weight = jnp.sum(weight, axis=1, keepdims=True)
    clip = jnp.maximum(1.0, jnp.sqrt(row_avg * weight / (count * float(D))))
    scale = learn_rate * jnp.sqrt(row_avg) / clip
    for c in range(TILES):
        root = scale / jnp.sqrt(new_cols_ref[:, tile(c)])
        for m in range(MATS):
            factor[m, :, tile(c)] = jnp.broadcast_to(root[m : m + 1, :], (8, LANES))

    eye = diagonal()
    for s in range(CAP):
        new = to_column(new_rows_ref[s : s + 1, :], eye)
        inverse[s] = jnp.broadcast_to(1.0 / jnp.sqrt(jnp.where(s < owned, new, 1.0)), (SUB, LANES))

    @pl.loop(0, owned)
    def _(s):
        m = matrix_ref[first + s]
        inv = inverse[s]
        for c in range(TILES):
            f = factor[m, :, tile(c)]
            change = grad_ref[s, :, tile(c)] * inv * jnp.concatenate([f, f], axis=0)
            out_ref[c, s] = (param_ref[s, :, tile(c)].astype(F32) - change).astype(BF16)


def update(block_start, block_matrix, step, grad, param, new_rows, total, col_state):
    return pl.pallas_call(
        update_kernel,
        out_shape=(
            jax.ShapeDtypeStruct((N_SHARD, CAP, SUB, LANES), BF16),
            jax.ShapeDtypeStruct((MATS, D), F32),
        ),
        in_specs=[SMEM, SMEM, SMEM, VMEM, VMEM, VMEM, VMEM, VMEM],
        out_specs=(VMEM, VMEM),
        scratch_shapes=[
            pltpu.VMEM((MATS, 8, D), F32),
            pltpu.VMEM((CAP, SUB, LANES), F32),
        ],
        compiler_params=pltpu.CompilerParams(vmem_limit_bytes=16 << 20),
        cost_estimate=pl.CostEstimate(flops=4000000, bytes_accessed=2400000, transcendentals=0),
        name="update",
    )(block_start, block_matrix, step, grad, param, new_rows, total, col_state)


def pack_kernel(table_ref, slots_ref, *out_refs):
    for b in range(NB):
        out_refs[b // PART][b % PART] = slots_ref[table_ref[b // LANES, b % LANES]]


def pack(table, slots):
    return pl.pallas_call(
        pack_kernel,
        out_shape=[jax.ShapeDtypeStruct((PART, SUB, LANES), BF16)] * PARTS,
        in_specs=[SMEM, VMEM],
        out_specs=[VMEM] * PARTS,
        compiler_params=pltpu.CompilerParams(vmem_limit_bytes=4 << 20),
        cost_estimate=pl.CostEstimate(flops=2000000, bytes_accessed=1200000, transcendentals=0),
        name="pack",
    )(table, slots.reshape(N_SHARD * CAP, SUB, LANES))


def place_kernel(where, *refs):
    pieces, out_ref, sems = refs[: len(where)], refs[-2], refs[-1]
    at = lax.axis_index("dp")
    copies = []
    for k, ((part, behind), piece) in enumerate(zip(where, pieces)):
        source = lax.rem(at + (DP - behind) % DP, DP)
        row = pl.multiple_of(source * SUB, SUB)
        target = out_ref.at[pl.ds(part * PART, PART), pl.ds(row, SUB), :]
        copies.append(pltpu.make_async_copy(piece, target, sems.at[k]))
    for copy in copies:
        copy.start()
    for copy in copies:
        copy.wait()


def place(where, pieces, out=None):
    n = len(pieces)
    return pl.pallas_call(
        functools.partial(place_kernel, where),
        out_shape=jax.ShapeDtypeStruct((NB, DP * SUB, LANES), BF16),
        in_specs=[ANY] * (n if out is None else n + 1),
        out_specs=ANY,
        scratch_shapes=[pltpu.SemaphoreType.DMA((n,))],
        input_output_aliases={} if out is None else {n: 0},
        compiler_params=pltpu.CompilerParams(vmem_limit_bytes=1 << 20),
        cost_estimate=pl.CostEstimate(flops=2000000, bytes_accessed=2400000, transcendentals=0),
        name="place",
    )(*pieces, *(() if out is None else (out,)))


def moved(x, axis, by):
    n = lax.axis_size(axis)
    return lax.ppermute(x, axis, [(i, (i + by) % n) for i in range(n)])


def fold_kernel(parts_ref, out_ref):
    total = parts_ref[0]
    for k in range(1, parts_ref.shape[0]):
        total = total + parts_ref[k]
    for k in range(out_ref.shape[0]):
        out_ref[k] = total


def fold(parts, copies):
    return pl.pallas_call(
        fold_kernel,
        out_shape=jax.ShapeDtypeStruct((copies, 8, LANES), F32),
        in_specs=[VMEM],
        out_specs=VMEM,
        compiler_params=pltpu.CompilerParams(vmem_limit_bytes=2 << 20),
        cost_estimate=pl.CostEstimate(flops=1000000000, bytes_accessed=4000000, transcendentals=0),
        name="fold",
    )(parts)


def summed(part):
    tiles, rest = SHARD, "dp"
    own = lax.all_to_all(part, tiles, 0, 0, tiled=True)
    own = lax.all_to_all(fold(own, N_SHARD * DP // TILES), rest, 0, 0, tiled=True)
    return lax.all_to_all(fold(own, TILES), tiles, 0, 0, tiled=True)


def body(grad, param, row_state, col_state, block_start, block_matrix, step):
    part, new_rows, table = stats(block_start, block_matrix, step, grad, row_state)
    total = summed(part)
    slots, new_cols = update(
        block_start, block_matrix, step, grad, param, new_rows, total, col_state
    )
    slots = lax.all_to_all(slots, SHARD, 0, 0, tiled=True)
    held = {}
    for part, piece in enumerate(pack(table, slots)):
        held[part, 0] = piece
    for hop in range(1, DP // 2 + 1):
        for part in range(PARTS):
            for way in (1, -1):
                if hop == DP // 2 and way != (1 if part == 0 else -1):
                    continue
                held[part, way * hop] = moved(held[part, way * (hop - 1)], "dp", way)
    out = None
    for hops in ((0, 1, 2), (3,), (4,)):
        now = [k for k in held if abs(k[1]) in hops]
        out = place(tuple(now), [held[k] for k in now], out)
    return (out.reshape(NB * DP * SUB, LANES), new_rows, new_cols)


def solution(mesh):
    finer = Mesh(
        mesh.devices.reshape(4, 4, 2, mesh.shape["dp"]), ("shard_0", "shard_1", "shard_2", "dp")
    )
    in_specs = (P(SHARD, "dp", None), P(SHARD, "dp", None), P(SHARD, "dp"), P(), P(), P(), P())
    out_specs = (P(None, SHARD), P(SHARD, "dp"), P())
    return jax.shard_map(body, mesh=finer, in_specs=in_specs, out_specs=out_specs, check_vma=False)
```

```python
import functools

import jax
import jax.numpy as jnp
from jax import lax
from jax.experimental import pallas as pl
from jax.experimental.pallas import tpu as pltpu
from jax.sharding import Mesh
from jax.sharding import PartitionSpec as P

D = 4096
FF = 10240
ROWS = (D, D, FF)
MATS = 3
NB = 144
CAP = 9
N_SHARD = 32
SUB = 16
LANES = 128
TILES = D // LANES
PARTS = 2
PART = NB // PARTS
DP = 8
SHARD = ("shard_0", "shard_1", "shard_2")
F32 = jnp.float32
BF16 = jnp.bfloat16


SMEM = pl.BlockSpec(memory_space=pltpu.SMEM)
VMEM = pl.BlockSpec(memory_space=pltpu.VMEM)
ANY = pl.BlockSpec(memory_space=pl.ANY)
MOST_VMEM = 62 << 20


def owned_range(start_ref):
    shard = (lax.axis_index("shard_0") * 4 + lax.axis_index("shard_1")) * 2 + lax.axis_index("shard_2")
    first = start_ref[shard]
    end = jnp.where(shard == N_SHARD - 1, NB, start_ref[jnp.minimum(shard + 1, N_SHARD - 1)])
    return first, end - first


def decay_rate(step_ref, shape):
    t = jnp.full(shape, step_ref[0].astype(F32))
    return 1.0 - jnp.exp(-0.8 * jnp.log(t))


def diagonal():
    shape = (SUB, SUB)
    return lax.broadcasted_iota(jnp.int32, shape, 0) == lax.broadcasted_iota(jnp.int32, shape, 1)


def to_column(row, eye):
    return jnp.sum(jnp.where(eye, jnp.broadcast_to(row, (SUB, SUB)), 0.0), axis=1, keepdims=True)


def to_row(column, eye):
    return jnp.sum(jnp.where(eye, jnp.broadcast_to(column, (SUB, SUB)), 0.0), axis=0, keepdims=True)


def tile(c):
    return slice(c * LANES, (c + 1) * LANES)


def decay_kernel(step_ref, decay_ref):
    decay_ref[...] = decay_rate(step_ref, decay_ref.shape)


def decay_of(step):
    return pl.pallas_call(
        decay_kernel,
        out_shape=jax.ShapeDtypeStruct((8, LANES), F32),
        in_specs=[SMEM],
        out_specs=VMEM,
        compiler_params=pltpu.CompilerParams(vmem_limit_bytes=2 << 20),
        cost_estimate=pl.CostEstimate(flops=1000000000, bytes_accessed=4000000, transcendentals=0),
        name="decay",
    )(step)


def stats_kernel(
    start_ref, matrix_ref, decay_ref, grad_ref, row_state_ref,
    part_ref, new_rows_ref, table_ref,
    sums, row_sums, inverse, row_total,
):
    first, owned = owned_range(start_ref)

    sums[...] = jnp.zeros_like(sums)
    row_total[...] = jnp.zeros_like(row_total)
    shape = (8, LANES)
    block = lax.broadcasted_iota(jnp.int32, shape, 0) * LANES + lax.broadcasted_iota(jnp.int32, shape, 1)
    slot = block
    for d in range(1, N_SHARD):
        slot = slot + jnp.where(block >= start_ref[d], CAP - (start_ref[d] - start_ref[d - 1]), 0)
    table_ref[...] = slot
    @pl.loop(0, owned)
    def _(s):
        total = jnp.zeros((SUB, LANES), F32)
        for c in range(TILES):
            x = grad_ref[s, :, tile(c)]
            total = total + x * x
        row_sums[s] = total

    eye = diagonal()
    decay = jnp.broadcast_to(decay_ref[:1, :1], (SUB, 1))
    for s in range(CAP):
        mean = jnp.sum(row_sums[s], axis=1, keepdims=True) / D
        state = to_column(row_state_ref[s : s + 1, :], eye)
        new = jnp.where(s < owned, decay * state + (1.0 - decay) * mean, 0.0)
        new_rows_ref[s : s + 1, :] = to_row(new, eye)
        inverse[s] = jnp.broadcast_to(jnp.where(s < owned, 1.0 / new, 0.0), (SUB, LANES))
        row_sums[s] = jnp.broadcast_to(new, (SUB, LANES))

    @pl.loop(0, owned)
    def _(s):
        m = matrix_ref[first + s]
        inv = inverse[s]
        new = row_sums[s]
        row_total[m] += new[:8] + new[8:]
        for c in range(TILES):
            x = grad_ref[s, :, tile(c)]
            sq = x * x
            quot = sq * inv
            sums[m, :, tile(c)] += sq[:8] + sq[8:]
            sums[MATS + m, :, tile(c)] += quot[:8] + quot[8:]

    for c in range(TILES):
        for m in range(MATS):
            part_ref[c, m : m + 1, :] = jnp.sum(sums[m, :, tile(c)], axis=0, keepdims=True)
            part_ref[c, 4 + m : 5 + m, :] = jnp.sum(sums[MATS + m, :, tile(c)], axis=0, keepdims=True)
        row = jnp.sum(row_total[c], axis=0, keepdims=True) if c < MATS else jnp.zeros((1, LANES), F32)
        part_ref[c, 3:4, :] = row
        part_ref[c, 7:8, :] = jnp.zeros((1, LANES), F32)


def stats(block_start, block_matrix, decay, grad, row_state):
    return pl.pallas_call(
        stats_kernel,
        out_shape=(
            jax.ShapeDtypeStruct((TILES, 8, LANES), F32),
            jax.ShapeDtypeStruct((CAP, SUB), F32),
            jax.ShapeDtypeStruct((8, LANES), jnp.int32),
        ),
        in_specs=[SMEM, SMEM, VMEM, VMEM, VMEM],
        out_specs=(VMEM, VMEM, VMEM),
        scratch_shapes=[
            pltpu.VMEM((2 * MATS, 8, D), F32),
            pltpu.VMEM((CAP, SUB, LANES), F32),
            pltpu.VMEM((CAP, SUB, LANES), F32),
            pltpu.VMEM((MATS, 8, LANES), F32),
        ],
        compiler_params=pltpu.CompilerParams(vmem_limit_bytes=16 << 20),
        cost_estimate=pl.CostEstimate(flops=4000000, bytes_accessed=2400000, transcendentals=0),
        name="stats",
    )(block_start, block_matrix, decay, grad, row_state)


def update_kernel(
    start_ref, matrix_ref, step_ref, grad_ref, param_ref, new_rows_ref, total_ref, col_state_ref,
    out_ref, new_cols_ref,
    factor, inverse,
):
    first, owned = owned_range(start_ref)
    matrix = lax.broadcasted_iota(jnp.int32, (MATS, 1), 0)
    count = jnp.where(matrix == 2, float(ROWS[2]), float(ROWS[0]))
    decay = decay_rate(step_ref, (MATS, 1))
    t = jnp.full((MATS, 1), step_ref[0].astype(F32))
    learn_rate = 1.0 / jnp.sqrt(jnp.maximum(t, 10000.0))
    row_avg = jnp.where(
        matrix == 0, total_ref[0, 3:4, :1], jnp.where(matrix == 1, total_ref[1, 3:4, :1], total_ref[2, 3:4, :1])
    ) / count
    weight = jnp.zeros((MATS, LANES), F32)
    for c in range(TILES):
        new = decay * col_state_ref[:, tile(c)] + (1.0 - decay) * total_ref[c, :MATS, :] / count
        new_cols_ref[:, tile(c)] = new
        weight = weight + total_ref[c, 4 : 4 + MATS, :] / new
    weight = jnp.sum(weight, axis=1, keepdims=True)
    clip = jnp.maximum(1.0, jnp.sqrt(row_avg * weight / (count * float(D))))
    scale = learn_rate * jnp.sqrt(row_avg) / clip
    for c in range(TILES):
        root = scale / jnp.sqrt(new_cols_ref[:, tile(c)])
        for m in range(MATS):
            factor[m, :, tile(c)] = jnp.broadcast_to(root[m : m + 1, :], (8, LANES))

    eye = diagonal()
    for s in range(CAP):
        new = to_column(new_rows_ref[s : s + 1, :], eye)
        inverse[s] = jnp.broadcast_to(1.0 / jnp.sqrt(jnp.where(s < owned, new, 1.0)), (SUB, LANES))

    @pl.loop(0, owned)
    def _(s):
        m = matrix_ref[first + s]
        inv = inverse[s]
        for c in range(TILES):
            f = factor[m, :, tile(c)]
            change = grad_ref[s, :, tile(c)] * inv * jnp.concatenate([f, f], axis=0)
            out_ref[c, s] = (param_ref[s, :, tile(c)].astype(F32) - change).astype(BF16)


def update(block_start, block_matrix, step, grad, param, new_rows, total, col_state):
    return pl.pallas_call(
        update_kernel,
        out_shape=(
            jax.ShapeDtypeStruct((N_SHARD, CAP, SUB, LANES), BF16),
            jax.ShapeDtypeStruct((MATS, D), F32),
        ),
        in_specs=[SMEM, SMEM, SMEM, VMEM, VMEM, VMEM, VMEM, VMEM],
        out_specs=(VMEM, VMEM),
        scratch_shapes=[
            pltpu.VMEM((MATS, 8, D), F32),
            pltpu.VMEM((CAP, SUB, LANES), F32),
        ],
        compiler_params=pltpu.CompilerParams(vmem_limit_bytes=16 << 20),
        cost_estimate=pl.CostEstimate(flops=4000000, bytes_accessed=2400000, transcendentals=0),
        name="update",
    )(block_start, block_matrix, step, grad, param, new_rows, total, col_state)


def pack_kernel(table_ref, slots_ref, *out_refs):
    for b in range(NB):
        out_refs[b // PART][b % PART] = slots_ref[table_ref[b // LANES, b % LANES]]


def pack(table, slots):
    return pl.pallas_call(
        pack_kernel,
        out_shape=[jax.ShapeDtypeStruct((PART, SUB, LANES), BF16)] * PARTS,
        in_specs=[SMEM, VMEM],
        out_specs=[VMEM] * PARTS,
        compiler_params=pltpu.CompilerParams(vmem_limit_bytes=4 << 20),
        cost_estimate=pl.CostEstimate(flops=2000000, bytes_accessed=1200000, transcendentals=0),
        name="pack",
    )(table, slots.reshape(N_SHARD * CAP, SUB, LANES))


def place_kernel(where, *refs):
    pieces, out_ref, sems = refs[: len(where)], refs[-2], refs[-1]
    at = lax.axis_index("dp")
    copies = []
    for k, ((part, behind), piece) in enumerate(zip(where, pieces)):
        source = lax.rem(at + (DP - behind) % DP, DP)
        row = pl.multiple_of(source * SUB, SUB)
        target = out_ref.at[pl.ds(part * PART, PART), pl.ds(row, SUB), :]
        copies.append(pltpu.make_async_copy(piece, target, sems.at[k]))
    for copy in copies:
        copy.start()
    for copy in copies:
        copy.wait()


def place(where, pieces, out=None):
    n = len(pieces)
    return pl.pallas_call(
        functools.partial(place_kernel, where),
        out_shape=jax.ShapeDtypeStruct((NB, DP * SUB, LANES), BF16),
        in_specs=[ANY] * (n if out is None else n + 1),
        out_specs=ANY,
        scratch_shapes=[pltpu.SemaphoreType.DMA((n,))],
        input_output_aliases={} if out is None else {n: 0},
        compiler_params=pltpu.CompilerParams(vmem_limit_bytes=1 << 20),
        cost_estimate=pl.CostEstimate(flops=2000000, bytes_accessed=2400000, transcendentals=0),
        name="place",
    )(*pieces, *(() if out is None else (out,)))


def moved(x, axis, by):
    n = lax.axis_size(axis)
    return lax.ppermute(x, axis, [(i, (i + by) % n) for i in range(n)])


def fold_kernel(parts_ref, out_ref):
    total = parts_ref[0]
    for k in range(1, parts_ref.shape[0]):
        total = total + parts_ref[k]
    for k in range(out_ref.shape[0]):
        out_ref[k] = total


def fold(parts, copies):
    return pl.pallas_call(
        fold_kernel,
        out_shape=jax.ShapeDtypeStruct((copies, 8, LANES), F32),
        in_specs=[VMEM],
        out_specs=VMEM,
        compiler_params=pltpu.CompilerParams(vmem_limit_bytes=2 << 20),
        cost_estimate=pl.CostEstimate(flops=1000000000, bytes_accessed=4000000, transcendentals=0),
        name="fold",
    )(parts)


def summed(part):
    tiles, rest = SHARD, "dp"
    own = lax.all_to_all(part, tiles, 0, 0, tiled=True)
    own = lax.all_to_all(fold(own, N_SHARD * DP // TILES), rest, 0, 0, tiled=True)
    return lax.all_to_all(fold(own, TILES), tiles, 0, 0, tiled=True)


def body(grad, param, row_state, col_state, block_start, block_matrix, step):
    part, new_rows, table = stats(block_start, block_matrix, decay_of(step), grad, row_state)
    total = summed(part)
    slots, new_cols = update(
        block_start, block_matrix, step, grad, param, new_rows, total, col_state
    )
    slots = lax.all_to_all(slots, SHARD, 0, 0, tiled=True)
    held = {}
    for part, piece in enumerate(pack(table, slots)):
        held[part, 0] = piece
    for hop in range(1, DP // 2 + 1):
        for part in range(PARTS):
            for way in (1, -1):
                if hop == DP // 2 and way != (1 if part == 0 else -1):
                    continue
                held[part, way * hop] = moved(held[part, way * (hop - 1)], "dp", way)
    out = None
    for hops in ((0, 1, 2), (3,), (4,)):
        now = [k for k in held if abs(k[1]) in hops]
        out = place(tuple(now), [held[k] for k in now], out)
    return (out.reshape(NB * DP * SUB, LANES), new_rows, new_cols)


def solution(mesh):
    finer = Mesh(
        mesh.devices.reshape(4, 4, 2, mesh.shape["dp"]), ("shard_0", "shard_1", "shard_2", "dp")
    )
    in_specs = (P(SHARD, "dp", None), P(SHARD, "dp", None), P(SHARD, "dp"), P(), P(), P(), P())
    out_specs = (P(None, SHARD), P(SHARD, "dp"), P())
    return jax.shard_map(body, mesh=finer, in_specs=in_specs, out_specs=out_specs, check_vma=False)
```

```python
import functools

import jax
import jax.numpy as jnp
from jax import lax
from jax.experimental import pallas as pl
from jax.experimental.pallas import tpu as pltpu
from jax.sharding import Mesh
from jax.sharding import PartitionSpec as P

D = 4096
FF = 10240
ROWS = (D, D, FF)
MATS = 3
NB = 144
CAP = 9
N_SHARD = 32
SUB = 16
LANES = 128
TILES = D // LANES
PARTS = 2
PART = NB // PARTS
DP = 8
SHARD = ("shard_0", "shard_1", "shard_2")
F32 = jnp.float32
BF16 = jnp.bfloat16


SMEM = pl.BlockSpec(memory_space=pltpu.SMEM)
VMEM = pl.BlockSpec(memory_space=pltpu.VMEM)
ANY = pl.BlockSpec(memory_space=pl.ANY)


def owned_range(start_ref):
    shard = (lax.axis_index("shard_0") * 4 + lax.axis_index("shard_1")) * 2 + lax.axis_index("shard_2")
    first = start_ref[shard]
    end = jnp.where(shard == N_SHARD - 1, NB, start_ref[jnp.minimum(shard + 1, N_SHARD - 1)])
    return first, end - first


def diagonal():
    shape = (SUB, SUB)
    return lax.broadcasted_iota(jnp.int32, shape, 0) == lax.broadcasted_iota(jnp.int32, shape, 1)


def to_column(row, eye):
    return jnp.sum(jnp.where(eye, jnp.broadcast_to(row, (SUB, SUB)), 0.0), axis=1, keepdims=True)


def to_row(column, eye):
    return jnp.sum(jnp.where(eye, jnp.broadcast_to(column, (SUB, SUB)), 0.0), axis=0, keepdims=True)


def tile(c):
    return slice(c * LANES, (c + 1) * LANES)


def rates_kernel(step_ref, rates_ref):
    t = jnp.full((4, LANES), step_ref[0].astype(F32))
    rates_ref[:4, :] = 1.0 - jnp.exp(-0.8 * jnp.log(t))
    rates_ref[4:, :] = 1.0 / jnp.sqrt(jnp.maximum(t, 10000.0))


def rates_of(step):
    return pl.pallas_call(
        rates_kernel,
        out_shape=jax.ShapeDtypeStruct((8, LANES), F32),
        in_specs=[SMEM],
        out_specs=VMEM,
        compiler_params=pltpu.CompilerParams(vmem_limit_bytes=2 << 20),
        cost_estimate=pl.CostEstimate(flops=1000000000, bytes_accessed=4000000, transcendentals=0),
        name="rates",
    )(step)


def stats_kernel(
    start_ref, matrix_ref, rates_ref, grad_ref, row_state_ref,
    part_ref, new_rows_out, table_ref,
    sums, row_sums, inverse, row_total, new_rows_ref, sem,
):
    first, owned = owned_range(start_ref)

    sums[...] = jnp.zeros_like(sums)
    row_total[...] = jnp.zeros_like(row_total)
    shape = (8, LANES)
    block = lax.broadcasted_iota(jnp.int32, shape, 0) * LANES + lax.broadcasted_iota(jnp.int32, shape, 1)
    slot = block
    for d in range(1, N_SHARD):
        slot = slot + jnp.where(block >= start_ref[d], CAP - (start_ref[d] - start_ref[d - 1]), 0)
    table_ref[...] = slot
    @pl.loop(0, owned)
    def _(s):
        total = jnp.zeros((SUB, LANES), F32)
        for c in range(TILES):
            x = grad_ref[s, :, tile(c)]
            total = total + x * x
        row_sums[s] = total

    eye = diagonal()
    decay = jnp.broadcast_to(rates_ref[:1, :1], (SUB, 1))
    for s in range(CAP):
        mean = jnp.sum(row_sums[s], axis=1, keepdims=True) / D
        state = to_column(row_state_ref[s : s + 1, :], eye)
        new = jnp.where(s < owned, decay * state + (1.0 - decay) * mean, 0.0)
        new_rows_ref[s : s + 1, :] = to_row(new, eye)
        inverse[s] = jnp.broadcast_to(jnp.where(s < owned, 1.0 / new, 0.0), (SUB, LANES))
        row_sums[s] = jnp.broadcast_to(new, (SUB, LANES))
    leaving = pltpu.make_async_copy(new_rows_ref, new_rows_out, sem)
    leaving.start()

    @pl.loop(0, owned)
    def _(s):
        m = matrix_ref[first + s]
        inv = inverse[s]
        new = row_sums[s]
        row_total[m] += new[:8] + new[8:]
        for c in range(TILES):
            x = grad_ref[s, :, tile(c)]
            sq = x * x
            quot = sq * inv
            sums[m, :, tile(c)] += sq[:8] + sq[8:]
            sums[MATS + m, :, tile(c)] += quot[:8] + quot[8:]

    for c in range(TILES):
        for m in range(MATS):
            part_ref[c, m : m + 1, :] = jnp.sum(sums[m, :, tile(c)], axis=0, keepdims=True)
            part_ref[c, 4 + m : 5 + m, :] = jnp.sum(sums[MATS + m, :, tile(c)], axis=0, keepdims=True)
        row = jnp.sum(row_total[c], axis=0, keepdims=True) if c < MATS else jnp.zeros((1, LANES), F32)
        part_ref[c, 3:4, :] = row
        part_ref[c, 7:8, :] = jnp.zeros((1, LANES), F32)
    leaving.wait()


def stats(block_start, block_matrix, rates, grad, row_state):
    return pl.pallas_call(
        stats_kernel,
        out_shape=(
            jax.ShapeDtypeStruct((TILES, 8, LANES), F32),
            jax.ShapeDtypeStruct((CAP, SUB), F32),
            jax.ShapeDtypeStruct((8, LANES), jnp.int32),
        ),
        in_specs=[SMEM, SMEM, VMEM, VMEM, VMEM],
        out_specs=(VMEM, ANY, VMEM),
        scratch_shapes=[
            pltpu.VMEM((2 * MATS, 8, D), F32),
            pltpu.VMEM((CAP, SUB, LANES), F32),
            pltpu.VMEM((CAP, SUB, LANES), F32),
            pltpu.VMEM((MATS, 8, LANES), F32),
            pltpu.VMEM((CAP, SUB), F32),
            pltpu.SemaphoreType.DMA,
        ],
        compiler_params=pltpu.CompilerParams(vmem_limit_bytes=16 << 20),
        cost_estimate=pl.CostEstimate(flops=4000000, bytes_accessed=2400000, transcendentals=0),
        name="stats",
    )(block_start, block_matrix, rates, grad, row_state)


def update_kernel(
    start_ref, matrix_ref, rates_ref, grad_ref, param_ref, new_rows_ref, total_ref, col_state_ref,
    out_ref, new_cols_out,
    factor, inverse, new_cols_ref, sem,
):
    first, owned = owned_range(start_ref)
    matrix = lax.broadcasted_iota(jnp.int32, (MATS, 1), 0)
    count = jnp.where(matrix == 2, float(ROWS[2]), float(ROWS[0]))
    decay = rates_ref[:MATS, :1]
    learn_rate = rates_ref[4 : 4 + MATS, :1]
    row_avg = jnp.where(
        matrix == 0, total_ref[0, 3:4, :1], jnp.where(matrix == 1, total_ref[1, 3:4, :1], total_ref[2, 3:4, :1])
    ) / count
    weight = jnp.zeros((MATS, LANES), F32)
    for c in range(TILES):
        new = decay * col_state_ref[:, tile(c)] + (1.0 - decay) * total_ref[c, :MATS, :] / count
        new_cols_ref[:, tile(c)] = new
        weight = weight + total_ref[c, 4 : 4 + MATS, :] / new
    leaving = pltpu.make_async_copy(new_cols_ref, new_cols_out, sem)
    leaving.start()
    weight = jnp.sum(weight, axis=1, keepdims=True)
    clip = jnp.maximum(1.0, jnp.sqrt(row_avg * weight / (count * float(D))))
    scale = learn_rate * jnp.sqrt(row_avg) / clip
    for c in range(TILES):
        root = scale / jnp.sqrt(new_cols_ref[:, tile(c)])
        for m in range(MATS):
            factor[m, :, tile(c)] = jnp.broadcast_to(root[m : m + 1, :], (8, LANES))

    eye = diagonal()
    for s in range(CAP):
        new = to_column(new_rows_ref[s : s + 1, :], eye)
        inverse[s] = jnp.broadcast_to(1.0 / jnp.sqrt(jnp.where(s < owned, new, 1.0)), (SUB, LANES))

    @pl.loop(0, owned)
    def _(s):
        m = matrix_ref[first + s]
        inv = inverse[s]
        for c in range(TILES):
            f = factor[m, :, tile(c)]
            change = grad_ref[s, :, tile(c)] * inv * jnp.concatenate([f, f], axis=0)
            out_ref[c, s] = (param_ref[s, :, tile(c)].astype(F32) - change).astype(BF16)

    leaving.wait()


def update(block_start, block_matrix, rates, grad, param, new_rows, total, col_state):
    return pl.pallas_call(
        update_kernel,
        out_shape=(
            jax.ShapeDtypeStruct((N_SHARD, CAP, SUB, LANES), BF16),
            jax.ShapeDtypeStruct((MATS, D), F32),
        ),
        in_specs=[SMEM, SMEM, VMEM, VMEM, VMEM, VMEM, VMEM, VMEM],
        out_specs=(VMEM, ANY),
        scratch_shapes=[
            pltpu.VMEM((MATS, 8, D), F32),
            pltpu.VMEM((CAP, SUB, LANES), F32),
            pltpu.VMEM((MATS, D), F32),
            pltpu.SemaphoreType.DMA,
        ],
        compiler_params=pltpu.CompilerParams(vmem_limit_bytes=16 << 20),
        cost_estimate=pl.CostEstimate(flops=4000000, bytes_accessed=2400000, transcendentals=0),
        name="update",
    )(block_start, block_matrix, rates, grad, param, new_rows, total, col_state)


def pack_kernel(table_ref, slots_ref, *out_refs):
    for b in range(NB):
        out_refs[b // PART][b % PART] = slots_ref[table_ref[b // LANES, b % LANES]]


def pack(table, slots):
    return pl.pallas_call(
        pack_kernel,
        out_shape=[jax.ShapeDtypeStruct((PART, SUB, LANES), BF16)] * PARTS,
        in_specs=[SMEM, VMEM],
        out_specs=[VMEM] * PARTS,
        compiler_params=pltpu.CompilerParams(vmem_limit_bytes=4 << 20),
        cost_estimate=pl.CostEstimate(flops=2000000, bytes_accessed=1200000, transcendentals=0),
        name="pack",
    )(table, slots.reshape(N_SHARD * CAP, SUB, LANES))


def place_kernel(where, *refs):
    pieces, out_ref, sems = refs[: len(where)], refs[-2], refs[-1]
    at = lax.axis_index("dp")
    copies = []
    for k, ((part, behind), piece) in enumerate(zip(where, pieces)):
        source = lax.rem(at + (DP - behind) % DP, DP)
        row = pl.multiple_of(source * SUB, SUB)
        target = out_ref.at[pl.ds(part * PART, PART), pl.ds(row, SUB), :]
        copies.append(pltpu.make_async_copy(piece, target, sems.at[k]))
    for copy in copies:
        copy.start()
    for copy in copies:
        copy.wait()


def place(where, pieces, out=None):
    n = len(pieces)
    return pl.pallas_call(
        functools.partial(place_kernel, where),
        out_shape=jax.ShapeDtypeStruct((NB, DP * SUB, LANES), BF16),
        in_specs=[ANY] * (n if out is None else n + 1),
        out_specs=ANY,
        scratch_shapes=[pltpu.SemaphoreType.DMA((n,))],
        input_output_aliases={} if out is None else {n: 0},
        compiler_params=pltpu.CompilerParams(vmem_limit_bytes=1 << 20),
        cost_estimate=pl.CostEstimate(flops=2000000, bytes_accessed=2400000, transcendentals=0),
        name="place",
    )(*pieces, *(() if out is None else (out,)))


def moved(x, axis, by):
    n = lax.axis_size(axis)
    return lax.ppermute(x, axis, [(i, (i + by) % n) for i in range(n)])


def fold_kernel(parts_ref, out_ref):
    total = parts_ref[0]
    for k in range(1, parts_ref.shape[0]):
        total = total + parts_ref[k]
    for k in range(out_ref.shape[0]):
        out_ref[k] = total


def fold(parts, copies):
    return pl.pallas_call(
        fold_kernel,
        out_shape=jax.ShapeDtypeStruct((copies, 8, LANES), F32),
        in_specs=[VMEM],
        out_specs=VMEM,
        compiler_params=pltpu.CompilerParams(vmem_limit_bytes=2 << 20),
        cost_estimate=pl.CostEstimate(flops=1000000000, bytes_accessed=4000000, transcendentals=0),
        name="fold",
    )(parts)


def summed(part):
    tiles, rest = SHARD, "dp"
    own = lax.all_to_all(part, tiles, 0, 0, tiled=True)
    own = lax.all_to_all(fold(own, N_SHARD * DP // TILES), rest, 0, 0, tiled=True)
    return lax.all_to_all(fold(own, TILES), tiles, 0, 0, tiled=True)


def body(grad, param, row_state, col_state, block_start, block_matrix, step):
    rates = rates_of(step)
    part, new_rows, table = stats(block_start, block_matrix, rates, grad, row_state)
    total = summed(part)
    slots, new_cols = update(
        block_start, block_matrix, rates, grad, param, new_rows, total, col_state
    )
    slots = lax.all_to_all(slots, SHARD, 0, 0, tiled=True)
    held = {}
    for part, piece in enumerate(pack(table, slots)):
        held[part, 0] = piece
    for hop in range(1, DP // 2 + 1):
        for part in range(PARTS):
            for way in (1, -1):
                if hop == DP // 2 and way != (1 if part == 0 else -1):
                    continue
                held[part, way * hop] = moved(held[part, way * (hop - 1)], "dp", way)
    out = None
    for hops in ((0, 1, 2), (3,), (4,)):
        now = [k for k in held if abs(k[1]) in hops]
        out = place(tuple(now), [held[k] for k in now], out)
    return (out.reshape(NB * DP * SUB, LANES), new_rows, new_cols)


def solution(mesh):
    finer = Mesh(
        mesh.devices.reshape(4, 4, 2, mesh.shape["dp"]), ("shard_0", "shard_1", "shard_2", "dp")
    )
    in_specs = (P(SHARD, "dp", None), P(SHARD, "dp", None), P(SHARD, "dp"), P(), P(), P(), P())
    out_specs = (P(None, SHARD), P(SHARD, "dp"), P())
    return jax.shard_map(body, mesh=finer, in_specs=in_specs, out_specs=out_specs, check_vma=False)
```

```python
import functools

import jax
import jax.numpy as jnp
from jax import lax
from jax.experimental import pallas as pl
from jax.experimental.pallas import tpu as pltpu
from jax.sharding import Mesh
from jax.sharding import PartitionSpec as P

D = 4096
FF = 10240
ROWS = (D, D, FF)
MATS = 3
NB = 144
CAP = 9
N_SHARD = 32
SUB = 16
LANES = 128
TILES = D // LANES
PARTS = 2
PART = NB // PARTS
COPIES = 3
DP = 8
SHARD = ("shard_0", "shard_1", "shard_2")
F32 = jnp.float32
BF16 = jnp.bfloat16


SMEM = pl.BlockSpec(memory_space=pltpu.SMEM)
VMEM = pl.BlockSpec(memory_space=pltpu.VMEM)
ANY = pl.BlockSpec(memory_space=pl.ANY)


def owned_range(start_ref):
    shard = (lax.axis_index("shard_0") * 4 + lax.axis_index("shard_1")) * 2 + lax.axis_index("shard_2")
    first = start_ref[shard]
    end = jnp.where(shard == N_SHARD - 1, NB, start_ref[jnp.minimum(shard + 1, N_SHARD - 1)])
    return first, end - first


def diagonal():
    shape = (SUB, SUB)
    return lax.broadcasted_iota(jnp.int32, shape, 0) == lax.broadcasted_iota(jnp.int32, shape, 1)


def to_column(row, eye):
    return jnp.sum(jnp.where(eye, jnp.broadcast_to(row, (SUB, SUB)), 0.0), axis=1, keepdims=True)


def to_row(column, eye):
    return jnp.sum(jnp.where(eye, jnp.broadcast_to(column, (SUB, SUB)), 0.0), axis=0, keepdims=True)


def tile(c):
    return slice(c * LANES, (c + 1) * LANES)


def rates_kernel(step_ref, rates_ref):
    t = jnp.full((4, LANES), step_ref[0].astype(F32))
    rates_ref[:4, :] = 1.0 - jnp.exp(-0.8 * jnp.log(t))
    rates_ref[4:, :] = 1.0 / jnp.sqrt(jnp.maximum(t, 10000.0))


def rates_of(step):
    return pl.pallas_call(
        rates_kernel,
        out_shape=jax.ShapeDtypeStruct((8, LANES), F32),
        in_specs=[SMEM],
        out_specs=VMEM,
        compiler_params=pltpu.CompilerParams(vmem_limit_bytes=2 << 20),
        cost_estimate=pl.CostEstimate(flops=1000000000, bytes_accessed=4000000, transcendentals=0),
        name="rates",
    )(step)


def stats_kernel(
    start_ref, matrix_ref, rates_ref, grad_ref, row_state_ref,
    part_ref, new_rows_out, table_ref,
    sums, row_sums, inverse, row_total, new_rows_ref, sem,
):
    first, owned = owned_range(start_ref)

    sums[...] = jnp.zeros_like(sums)
    row_total[...] = jnp.zeros_like(row_total)
    shape = (8, LANES)
    block = lax.broadcasted_iota(jnp.int32, shape, 0) * LANES + lax.broadcasted_iota(jnp.int32, shape, 1)
    slot = block
    for d in range(1, N_SHARD):
        slot = slot + jnp.where(block >= start_ref[d], CAP - (start_ref[d] - start_ref[d - 1]), 0)
    table_ref[...] = slot
    @pl.loop(0, owned)
    def _(s):
        total = jnp.zeros((SUB, LANES), F32)
        for c in range(TILES):
            x = grad_ref[s, :, tile(c)]
            total = total + x * x
        row_sums[s] = total

    eye = diagonal()
    decay = jnp.broadcast_to(rates_ref[:1, :1], (SUB, 1))
    for s in range(CAP):
        mean = jnp.sum(row_sums[s], axis=1, keepdims=True) / D
        state = to_column(row_state_ref[s : s + 1, :], eye)
        new = jnp.where(s < owned, decay * state + (1.0 - decay) * mean, 0.0)
        new_rows_ref[s : s + 1, :] = to_row(new, eye)
        inverse[s] = jnp.broadcast_to(jnp.where(s < owned, 1.0 / new, 0.0), (SUB, LANES))
        row_sums[s] = jnp.broadcast_to(new, (SUB, LANES))
    leaving = pltpu.make_async_copy(new_rows_ref, new_rows_out, sem)
    leaving.start()

    @pl.loop(0, owned)
    def _(s):
        m = matrix_ref[first + s]
        inv = inverse[s]
        new = row_sums[s]
        row_total[m] += new[:8] + new[8:]
        for c in range(TILES):
            x = grad_ref[s, :, tile(c)]
            sq = x * x
            quot = sq * inv
            sums[m, :, tile(c)] += sq[:8] + sq[8:]
            sums[MATS + m, :, tile(c)] += quot[:8] + quot[8:]

    for c in range(TILES):
        for m in range(MATS):
            part_ref[c, m : m + 1, :] = jnp.sum(sums[m, :, tile(c)], axis=0, keepdims=True)
            part_ref[c, 4 + m : 5 + m, :] = jnp.sum(sums[MATS + m, :, tile(c)], axis=0, keepdims=True)
        row = jnp.sum(row_total[c], axis=0, keepdims=True) if c < MATS else jnp.zeros((1, LANES), F32)
        part_ref[c, 3:4, :] = row
        part_ref[c, 7:8, :] = jnp.zeros((1, LANES), F32)
    leaving.wait()


def stats(block_start, block_matrix, rates, grad, row_state):
    return pl.pallas_call(
        stats_kernel,
        out_shape=(
            jax.ShapeDtypeStruct((TILES, 8, LANES), F32),
            jax.ShapeDtypeStruct((CAP, SUB), F32),
            jax.ShapeDtypeStruct((8, LANES), jnp.int32),
        ),
        in_specs=[SMEM, SMEM, VMEM, VMEM, VMEM],
        out_specs=(VMEM, ANY, VMEM),
        scratch_shapes=[
            pltpu.VMEM((2 * MATS, 8, D), F32),
            pltpu.VMEM((CAP, SUB, LANES), F32),
            pltpu.VMEM((CAP, SUB, LANES), F32),
            pltpu.VMEM((MATS, 8, LANES), F32),
            pltpu.VMEM((CAP, SUB), F32),
            pltpu.SemaphoreType.DMA,
        ],
        compiler_params=pltpu.CompilerParams(vmem_limit_bytes=16 << 20),
        cost_estimate=pl.CostEstimate(flops=4000000, bytes_accessed=2400000, transcendentals=0),
        name="stats",
    )(block_start, block_matrix, rates, grad, row_state)


def update_kernel(
    start_ref, matrix_ref, rates_ref, grad_ref, param_ref, new_rows_ref, total_ref, col_state_ref,
    out_ref, new_cols_out,
    factor, inverse, new_cols_ref, sem,
):
    first, owned = owned_range(start_ref)
    matrix = lax.broadcasted_iota(jnp.int32, (MATS, 1), 0)
    count = jnp.where(matrix == 2, float(ROWS[2]), float(ROWS[0]))
    decay = rates_ref[:MATS, :1]
    learn_rate = rates_ref[4 : 4 + MATS, :1]
    row_avg = jnp.where(
        matrix == 0, total_ref[0, 3:4, :1], jnp.where(matrix == 1, total_ref[1, 3:4, :1], total_ref[2, 3:4, :1])
    ) / count
    weight = jnp.zeros((MATS, LANES), F32)
    share = (1.0 - decay) / count
    for c in range(TILES):
        new = decay * col_state_ref[:, tile(c)] + share * total_ref[c, :MATS, :]
        new_cols_ref[:, tile(c)] = new
        weight = weight + total_ref[c, 4 : 4 + MATS, :] / new
    leaving = pltpu.make_async_copy(new_cols_ref, new_cols_out, sem)
    leaving.start()
    weight = jnp.sum(weight, axis=1, keepdims=True)
    clip = jnp.maximum(1.0, jnp.sqrt(row_avg * weight / (count * float(D))))
    scale = learn_rate * jnp.sqrt(row_avg) / clip
    for c in range(TILES):
        root = scale / jnp.sqrt(new_cols_ref[:, tile(c)])
        for m in range(MATS):
            factor[m, :, tile(c)] = jnp.broadcast_to(root[m : m + 1, :], (8, LANES))

    eye = diagonal()
    for s in range(CAP):
        new = to_column(new_rows_ref[s : s + 1, :], eye)
        inverse[s] = jnp.broadcast_to(1.0 / jnp.sqrt(jnp.where(s < owned, new, 1.0)), (SUB, LANES))

    @pl.loop(0, owned)
    def _(s):
        m = matrix_ref[first + s]
        inv = inverse[s]
        for c in range(TILES):
            f = factor[m, :, tile(c)]
            change = grad_ref[s, :, tile(c)] * inv * jnp.concatenate([f, f], axis=0)
            out_ref[c, s] = (param_ref[s, :, tile(c)].astype(F32) - change).astype(BF16)

    leaving.wait()


def update(block_start, block_matrix, rates, grad, param, new_rows, total, col_state):
    return pl.pallas_call(
        update_kernel,
        out_shape=(
            jax.ShapeDtypeStruct((N_SHARD, CAP, SUB, LANES), BF16),
            jax.ShapeDtypeStruct((MATS, D), F32),
        ),
        in_specs=[SMEM, SMEM, VMEM, VMEM, VMEM, VMEM, VMEM, VMEM],
        out_specs=(VMEM, ANY),
        scratch_shapes=[
            pltpu.VMEM((MATS, 8, D), F32),
            pltpu.VMEM((CAP, SUB, LANES), F32),
            pltpu.VMEM((MATS, D), F32),
            pltpu.SemaphoreType.DMA,
        ],
        compiler_params=pltpu.CompilerParams(vmem_limit_bytes=16 << 20),
        cost_estimate=pl.CostEstimate(flops=4000000, bytes_accessed=2400000, transcendentals=0),
        name="update",
    )(block_start, block_matrix, rates, grad, param, new_rows, total, col_state)


def pack_kernel(table_ref, slots_ref, *out_refs):
    for b in range(NB):
        out_refs[b // PART][b % PART] = slots_ref[table_ref[b // LANES, b % LANES]]


def pack(table, slots):
    return pl.pallas_call(
        pack_kernel,
        out_shape=[jax.ShapeDtypeStruct((PART, SUB, LANES), BF16)] * PARTS,
        in_specs=[SMEM, VMEM],
        out_specs=[VMEM] * PARTS,
        compiler_params=pltpu.CompilerParams(vmem_limit_bytes=4 << 20),
        cost_estimate=pl.CostEstimate(flops=2000000, bytes_accessed=1200000, transcendentals=0),
        name="pack",
    )(table, slots.reshape(N_SHARD * CAP, SUB, LANES))


def place_kernel(where, *refs):
    pieces, out_ref, sems = refs[: len(where)], refs[-2], refs[-1]
    at = lax.axis_index("dp")
    copies = []
    size = PART // COPIES
    for k, ((part, behind), piece) in enumerate(zip(where, pieces)):
        source = lax.rem(at + (DP - behind) % DP, DP)
        row = pl.multiple_of(source * SUB, SUB)
        for j in range(COPIES):
            target = out_ref.at[pl.ds(part * PART + j * size, size), pl.ds(row, SUB), :]
            copies.append(
                pltpu.make_async_copy(piece.at[pl.ds(j * size, size)], target, sems.at[k * COPIES + j])
            )
    for copy in copies:
        copy.start()
    for copy in copies:
        copy.wait()


def place(where, pieces, out=None):
    n = len(pieces)
    return pl.pallas_call(
        functools.partial(place_kernel, where),
        out_shape=jax.ShapeDtypeStruct((NB, DP * SUB, LANES), BF16),
        in_specs=[ANY] * (n if out is None else n + 1),
        out_specs=ANY,
        scratch_shapes=[pltpu.SemaphoreType.DMA((n * COPIES,))],
        input_output_aliases={} if out is None else {n: 0},
        compiler_params=pltpu.CompilerParams(vmem_limit_bytes=1 << 20),
        cost_estimate=pl.CostEstimate(flops=2000000, bytes_accessed=2400000, transcendentals=0),
        name="place",
    )(*pieces, *(() if out is None else (out,)))


def moved(x, axis, by):
    n = lax.axis_size(axis)
    return lax.ppermute(x, axis, [(i, (i + by) % n) for i in range(n)])


def fold_kernel(parts_ref, out_ref):
    total = parts_ref[0]
    for k in range(1, parts_ref.shape[0]):
        total = total + parts_ref[k]
    for k in range(out_ref.shape[0]):
        out_ref[k] = total


def fold(parts, copies):
    return pl.pallas_call(
        fold_kernel,
        out_shape=jax.ShapeDtypeStruct((copies, 8, LANES), F32),
        in_specs=[VMEM],
        out_specs=VMEM,
        compiler_params=pltpu.CompilerParams(vmem_limit_bytes=2 << 20),
        cost_estimate=pl.CostEstimate(flops=1000000000, bytes_accessed=4000000, transcendentals=0),
        name="fold",
    )(parts)


def summed(part):
    tiles, rest = SHARD, "dp"
    own = lax.all_to_all(part, tiles, 0, 0, tiled=True)
    own = lax.all_to_all(fold(own, N_SHARD * DP // TILES), rest, 0, 0, tiled=True)
    return lax.all_to_all(fold(own, TILES), tiles, 0, 0, tiled=True)


def body(grad, param, row_state, col_state, block_start, block_matrix, step):
    rates = rates_of(step)
    part, new_rows, table = stats(block_start, block_matrix, rates, grad, row_state)
    total = summed(part)
    slots, new_cols = update(
        block_start, block_matrix, rates, grad, param, new_rows, total, col_state
    )
    slots = lax.all_to_all(slots, SHARD, 0, 0, tiled=True)
    held = {}
    for part, piece in enumerate(pack(table, slots)):
        held[part, 0] = piece
    for hop in range(1, DP // 2 + 1):
        for part in range(PARTS):
            for way in (1, -1):
                if hop == DP // 2 and way != (1 if part == 0 else -1):
                    continue
                held[part, way * hop] = moved(held[part, way * (hop - 1)], "dp", way)
    out = None
    for hops in ((0, 1, 2), (3,), (4,)):
        now = [k for k in held if abs(k[1]) in hops]
        out = place(tuple(now), [held[k] for k in now], out)
    return (out.reshape(NB * DP * SUB, LANES), new_rows, new_cols)


def solution(mesh):
    finer = Mesh(
        mesh.devices.reshape(4, 4, 2, mesh.shape["dp"]), ("shard_0", "shard_1", "shard_2", "dp")
    )
    in_specs = (P(SHARD, "dp", None), P(SHARD, "dp", None), P(SHARD, "dp"), P(), P(), P(), P())
    out_specs = (P(None, SHARD), P(SHARD, "dp"), P())
    return jax.shard_map(body, mesh=finer, in_specs=in_specs, out_specs=out_specs, check_vma=False)
```

```python
import functools

import jax
import jax.numpy as jnp
from jax import lax
from jax.experimental import pallas as pl
from jax.experimental.pallas import tpu as pltpu
from jax.sharding import Mesh
from jax.sharding import PartitionSpec as P

D = 4096
FF = 10240
ROWS = (D, D, FF)
MATS = 3
NB = 144
CAP = 9
N_SHARD = 32
SUB = 16
LANES = 128
TILES = D // LANES
PARTS = 2
PART = NB // PARTS
DP = 8
SHARD = ("shard_0", "shard_1", "shard_2")
F32 = jnp.float32
BF16 = jnp.bfloat16


SMEM = pl.BlockSpec(memory_space=pltpu.SMEM)
VMEM = pl.BlockSpec(memory_space=pltpu.VMEM)
ANY = pl.BlockSpec(memory_space=pl.ANY)


def owned_range(start_ref):
    shard = (lax.axis_index("shard_0") * 4 + lax.axis_index("shard_1")) * 2 + lax.axis_index("shard_2")
    first = start_ref[shard]
    end = jnp.where(shard == N_SHARD - 1, NB, start_ref[jnp.minimum(shard + 1, N_SHARD - 1)])
    return first, end - first


def diagonal():
    shape = (SUB, SUB)
    return lax.broadcasted_iota(jnp.int32, shape, 0) == lax.broadcasted_iota(jnp.int32, shape, 1)


def to_column(row, eye):
    return jnp.sum(jnp.where(eye, jnp.broadcast_to(row, (SUB, SUB)), 0.0), axis=1, keepdims=True)


def to_row(column, eye):
    return jnp.sum(jnp.where(eye, jnp.broadcast_to(column, (SUB, SUB)), 0.0), axis=0, keepdims=True)


def tile(c):
    return slice(c * LANES, (c + 1) * LANES)


def rates_kernel(step_ref, rates_ref):
    t = jnp.full((4, LANES), step_ref[0].astype(F32))
    rates_ref[:4, :] = 1.0 - jnp.exp(-0.8 * jnp.log(t))
    rates_ref[4:, :] = 1.0 / jnp.sqrt(jnp.maximum(t, 10000.0))


def rates_of(step):
    return pl.pallas_call(
        rates_kernel,
        out_shape=jax.ShapeDtypeStruct((8, LANES), F32),
        in_specs=[SMEM],
        out_specs=VMEM,
        compiler_params=pltpu.CompilerParams(vmem_limit_bytes=2 << 20),
        cost_estimate=pl.CostEstimate(flops=1000000000, bytes_accessed=4000000, transcendentals=0),
        name="rates",
    )(step)


def stats_kernel(
    start_ref, matrix_ref, rates_ref, grad_ref, row_state_ref,
    part_ref, new_rows_out, table_ref,
    sums, row_sums, inverse, row_total, new_rows_ref, sem,
):
    first, owned = owned_range(start_ref)

    sums[...] = jnp.zeros_like(sums)
    row_total[...] = jnp.zeros_like(row_total)
    shape = (8, LANES)
    block = lax.broadcasted_iota(jnp.int32, shape, 0) * LANES + lax.broadcasted_iota(jnp.int32, shape, 1)
    slot = block
    for d in range(1, N_SHARD):
        slot = slot + jnp.where(block >= start_ref[d], CAP - (start_ref[d] - start_ref[d - 1]), 0)
    table_ref[...] = slot
    @pl.loop(0, owned)
    def _(s):
        total = jnp.zeros((SUB, LANES), F32)
        for c in range(TILES):
            x = grad_ref[s, :, tile(c)]
            total = total + x * x
        row_sums[s] = total

    eye = diagonal()
    decay = jnp.broadcast_to(rates_ref[:1, :1], (SUB, 1))
    for s in range(CAP):
        mean = jnp.sum(row_sums[s], axis=1, keepdims=True) / D
        state = to_column(row_state_ref[s : s + 1, :], eye)
        new = jnp.where(s < owned, decay * state + (1.0 - decay) * mean, 0.0)
        new_rows_ref[s : s + 1, :] = to_row(new, eye)
        inverse[s] = jnp.broadcast_to(jnp.where(s < owned, 1.0 / new, 0.0), (SUB, LANES))
        row_sums[s] = jnp.broadcast_to(new, (SUB, LANES))
    leaving = pltpu.make_async_copy(new_rows_ref, new_rows_out, sem)
    leaving.start()

    @pl.loop(0, owned)
    def _(s):
        m = matrix_ref[first + s]
        inv = inverse[s]
        new = row_sums[s]
        row_total[m] += new[:8] + new[8:]
        for c in range(TILES):
            x = grad_ref[s, :, tile(c)]
            sq = x * x
            quot = sq * inv
            sums[m, :, tile(c)] += sq[:8] + sq[8:]
            sums[MATS + m, :, tile(c)] += quot[:8] + quot[8:]

    for c in range(TILES):
        for m in range(MATS):
            part_ref[c, m : m + 1, :] = jnp.sum(sums[m, :, tile(c)], axis=0, keepdims=True)
            part_ref[c, 4 + m : 5 + m, :] = jnp.sum(sums[MATS + m, :, tile(c)], axis=0, keepdims=True)
        row = jnp.sum(row_total[c], axis=0, keepdims=True) if c < MATS else jnp.zeros((1, LANES), F32)
        part_ref[c, 3:4, :] = row
        part_ref[c, 7:8, :] = jnp.zeros((1, LANES), F32)
    leaving.wait()


def stats(block_start, block_matrix, rates, grad, row_state):
    return pl.pallas_call(
        stats_kernel,
        out_shape=(
            jax.ShapeDtypeStruct((TILES, 8, LANES), F32),
            jax.ShapeDtypeStruct((CAP, SUB), F32),
            jax.ShapeDtypeStruct((8, LANES), jnp.int32),
        ),
        in_specs=[SMEM, SMEM, VMEM, VMEM, VMEM],
        out_specs=(VMEM, ANY, VMEM),
        scratch_shapes=[
            pltpu.VMEM((2 * MATS, 8, D), F32),
            pltpu.VMEM((CAP, SUB, LANES), F32),
            pltpu.VMEM((CAP, SUB, LANES), F32),
            pltpu.VMEM((MATS, 8, LANES), F32),
            pltpu.VMEM((CAP, SUB), F32),
            pltpu.SemaphoreType.DMA,
        ],
        compiler_params=pltpu.CompilerParams(vmem_limit_bytes=16 << 20),
        cost_estimate=pl.CostEstimate(flops=4000000, bytes_accessed=2400000, transcendentals=0),
        name="stats",
    )(block_start, block_matrix, rates, grad, row_state)


def update_kernel(
    start_ref, matrix_ref, rates_ref, grad_ref, param_ref, new_rows_ref, total_ref, col_state_ref,
    out_ref, new_cols_out,
    factor, inverse, new_cols_ref, sem,
):
    first, owned = owned_range(start_ref)
    matrix = lax.broadcasted_iota(jnp.int32, (MATS, 1), 0)
    count = jnp.where(matrix == 2, float(ROWS[2]), float(ROWS[0]))
    decay = rates_ref[:MATS, :1]
    learn_rate = rates_ref[4 : 4 + MATS, :1]
    row_avg = jnp.where(
        matrix == 0, total_ref[0, 3:4, :1], jnp.where(matrix == 1, total_ref[1, 3:4, :1], total_ref[2, 3:4, :1])
    ) / count
    weight = jnp.zeros((MATS, LANES), F32)
    for c in range(TILES):
        new = decay * col_state_ref[:, tile(c)] + (1.0 - decay) * total_ref[c, :MATS, :] / count
        new_cols_ref[:, tile(c)] = new
        weight = weight + total_ref[c, 4 : 4 + MATS, :] / new
    leaving = pltpu.make_async_copy(new_cols_ref, new_cols_out, sem)
    leaving.start()
    weight = jnp.sum(weight, axis=1, keepdims=True)
    clip = jnp.maximum(1.0, jnp.sqrt(row_avg * weight / (count * float(D))))
    scale = learn_rate * jnp.sqrt(row_avg) / clip
    for c in range(TILES):
        root = scale / jnp.sqrt(new_cols_ref[:, tile(c)])
        for m in range(MATS):
            factor[m, :, tile(c)] = jnp.broadcast_to(root[m : m + 1, :], (8, LANES))

    eye = diagonal()
    for s in range(CAP):
        new = to_column(new_rows_ref[s : s + 1, :], eye)
        inverse[s] = jnp.broadcast_to(1.0 / jnp.sqrt(jnp.where(s < owned, new, 1.0)), (SUB, LANES))

    @pl.loop(0, owned)
    def _(s):
        m = matrix_ref[first + s]
        inv = inverse[s]
        for c in range(TILES):
            f = factor[m, :, tile(c)]
            change = grad_ref[s, :, tile(c)] * inv * jnp.concatenate([f, f], axis=0)
            out_ref[c, s] = (param_ref[s, :, tile(c)].astype(F32) - change).astype(BF16)

    leaving.wait()


def update(block_start, block_matrix, rates, grad, param, new_rows, total, col_state):
    return pl.pallas_call(
        update_kernel,
        out_shape=(
            jax.ShapeDtypeStruct((N_SHARD, CAP, SUB, LANES), BF16),
            jax.ShapeDtypeStruct((MATS, D), F32),
        ),
        in_specs=[SMEM, SMEM, VMEM, VMEM, VMEM, VMEM, VMEM, VMEM],
        out_specs=(VMEM, ANY),
        scratch_shapes=[
            pltpu.VMEM((MATS, 8, D), F32),
            pltpu.VMEM((CAP, SUB, LANES), F32),
            pltpu.VMEM((MATS, D), F32),
            pltpu.SemaphoreType.DMA,
        ],
        compiler_params=pltpu.CompilerParams(vmem_limit_bytes=16 << 20),
        cost_estimate=pl.CostEstimate(flops=4000000, bytes_accessed=2400000, transcendentals=0),
        name="update",
    )(block_start, block_matrix, rates, grad, param, new_rows, total, col_state)


def pack_kernel(table_ref, slots_ref, *out_refs):
    for b in range(NB):
        out_refs[b // PART][b % PART] = slots_ref[table_ref[b // LANES, b % LANES]]


def pack(table, slots):
    return pl.pallas_call(
        pack_kernel,
        out_shape=[jax.ShapeDtypeStruct((PART, SUB, LANES), BF16)] * PARTS,
        in_specs=[SMEM, VMEM],
        out_specs=[VMEM] * PARTS,
        compiler_params=pltpu.CompilerParams(vmem_limit_bytes=4 << 20),
        cost_estimate=pl.CostEstimate(flops=2000000, bytes_accessed=1200000, transcendentals=0),
        name="pack",
    )(table, slots.reshape(N_SHARD * CAP, SUB, LANES))


def place_kernel(where, *refs):
    pieces, out_ref, sems = refs[: len(where)], refs[-2], refs[-1]
    at = lax.axis_index("dp")
    copies = []
    for k, ((part, behind), piece) in enumerate(zip(where, pieces)):
        source = lax.rem(at + (DP - behind) % DP, DP)
        row = pl.multiple_of(source * SUB, SUB)
        target = out_ref.at[pl.ds(part * PART, PART), pl.ds(row, SUB), :]
        copies.append(pltpu.make_async_copy(piece, target, sems.at[k]))
    for copy in copies:
        copy.start()
    for copy in copies:
        copy.wait()


def place(where, pieces, out=None):
    n = len(pieces)
    return pl.pallas_call(
        functools.partial(place_kernel, where),
        out_shape=jax.ShapeDtypeStruct((NB, DP * SUB, LANES), BF16),
        in_specs=[ANY] * (n if out is None else n + 1),
        out_specs=ANY,
        scratch_shapes=[pltpu.SemaphoreType.DMA((n,))],
        input_output_aliases={} if out is None else {n: 0},
        compiler_params=pltpu.CompilerParams(vmem_limit_bytes=1 << 20),
        cost_estimate=pl.CostEstimate(flops=2000000, bytes_accessed=2400000, transcendentals=0),
        name="place",
    )(*pieces, *(() if out is None else (out,)))


def moved(x, axis, by):
    n = lax.axis_size(axis)
    return lax.ppermute(x, axis, [(i, (i + by) % n) for i in range(n)])


def fold_kernel(parts_ref, out_ref):
    total = parts_ref[0]
    for k in range(1, parts_ref.shape[0]):
        total = total + parts_ref[k]
    for k in range(out_ref.shape[0]):
        out_ref[k] = total


def fold(parts, copies):
    return pl.pallas_call(
        fold_kernel,
        out_shape=jax.ShapeDtypeStruct((copies, 8, LANES), F32),
        in_specs=[VMEM],
        out_specs=VMEM,
        compiler_params=pltpu.CompilerParams(vmem_limit_bytes=2 << 20),
        cost_estimate=pl.CostEstimate(flops=1000000000, bytes_accessed=4000000, transcendentals=0),
        name="fold",
    )(parts)


def summed(part):
    tiles, rest = SHARD, "dp"
    own = lax.all_to_all(part, tiles, 0, 0, tiled=True)
    own = lax.all_to_all(fold(own, N_SHARD * DP // TILES), rest, 0, 0, tiled=True)
    return lax.all_to_all(fold(own, TILES), tiles, 0, 0, tiled=True)


def body(grad, param, row_state, col_state, block_start, block_matrix, step):
    rates = rates_of(step)
    part, new_rows, table = stats(block_start, block_matrix, rates, grad, row_state)
    total = summed(part)
    slots, new_cols = update(
        block_start, block_matrix, rates, grad, param, new_rows, total, col_state
    )
    slots = lax.all_to_all(slots, SHARD, 0, 0, tiled=True)
    held = {}
    for part, piece in enumerate(pack(table, slots)):
        held[part, 0] = piece
    for hop in range(1, DP // 2 + 1):
        for part in range(PARTS):
            for way in (1, -1):
                if hop == DP // 2 and way != (1 if part == 0 else -1):
                    continue
                held[part, way * hop] = moved(held[part, way * (hop - 1)], "dp", way)
    out = None
    for hops in ((0, 1), (2, 3), (4,)):
        now = [k for k in held if abs(k[1]) in hops]
        out = place(tuple(now), [held[k] for k in now], out)
    return (out.reshape(NB * DP * SUB, LANES), new_rows, new_cols)


def solution(mesh):
    finer = Mesh(
        mesh.devices.reshape(4, 4, 2, mesh.shape["dp"]), ("shard_0", "shard_1", "shard_2", "dp")
    )
    in_specs = (P(SHARD, "dp", None), P(SHARD, "dp", None), P(SHARD, "dp"), P(), P(), P(), P())
    out_specs = (P(None, SHARD), P(SHARD, "dp"), P())
    return jax.shard_map(body, mesh=finer, in_specs=in_specs, out_specs=out_specs, check_vma=False)
```
